128 devices in a mesh: data: 1, fsdp: 128 (over z, y, x, core).
Axes of the slice: x: 4, y: 4, z: 4, core: 2. Of those that a mesh axis runs over, the one named last changes fastest.
Arguments:
- hidden: bfloat16 [8192, 640], P('data')
- targets: int32 [8192], P('data')
- w_out: bfloat16 [262144, 640], P('fsdp')
Outputs:
- output 1: float32 [1], P('data')
- output 2: float32 [8192, 640], P(('data', 'fsdp'))
- output 3: float32 [262144, 640], P(('data', 'fsdp'))
All inputs are finite; a program needn't handle non-finite values.
Results may differ from the reference program's by a relative error of at most 0.00115.
Values are sent between devices in bfloat16 or wider.
A program may use at most 1 GiB of HBM per device.

```python
import math
import jax
import jax.numpy as jnp
from jax import lax

GROUP_SIZE = 128
TOKENS_DEV = 64
VOCAB_SIZE = 262144
MODEL_DIM = 640

TOKENS = TOKENS_DEV * GROUP_SIZE
VOCAB_DEV = VOCAB_SIZE // GROUP_SIZE


def setup_inputs(seed: int = 0, part: int = 0) -> dict:
    base_key = jax.random.key(seed)
    shared_key, part_base = jax.random.split(base_key)
    part_key = jax.random.fold_in(part_base, part)
    noise_key, offset_key, perm_key = jax.random.split(part_key, 3)
    w_out = (jax.random.normal(shared_key, (VOCAB_SIZE, MODEL_DIM), jnp.float32) * MODEL_DIM ** -0.5).astype(jnp.bfloat16)
    positions = jnp.arange(TOKENS)
    offsets = jax.random.randint(offset_key, (TOKENS,), 0, VOCAB_DEV)
    offsets = jnp.where(positions == 0, 0, offsets)
    offsets = jnp.where(positions == GROUP_SIZE - 1, VOCAB_DEV - 1, offsets)
    targets = jax.random.permutation(perm_key, (positions % GROUP_SIZE) * VOCAB_DEV + offsets).astype(jnp.int32)
    boost = math.log(VOCAB_SIZE)
    hidden = jax.random.normal(noise_key, (TOKENS, MODEL_DIM), jnp.float32) + boost * w_out.astype(jnp.float32)[targets]
    return {"hidden": hidden.astype(jnp.bfloat16), "targets": targets, "w_out": w_out}


def reference(hidden, targets, w_out):
    hid_blocks = hidden.reshape(GROUP_SIZE, TOKENS_DEV, MODEL_DIM)
    tgt_blocks = targets.reshape(GROUP_SIZE, TOKENS_DEV)
    vocab_ids = jnp.arange(VOCAB_SIZE)[None, :]

    def scan_step(grad_w, blocks):
        hid_blk, tgt_blk = blocks
        logits = jnp.dot(hid_blk, w_out.T, preferred_element_type=jnp.float32)
        row_max = jnp.max(logits, axis=1, keepdims=True)
        log_norm = row_max + jnp.log(jnp.sum(jnp.exp(logits - row_max), axis=1, keepdims=True))
        tgt_hit = vocab_ids == tgt_blk[:, None]
        tgt_logit = jnp.sum(jnp.where(tgt_hit, logits, 0.0), axis=1, keepdims=True)
        probs = jnp.exp(logits - log_norm)
        grad_logits = ((probs - tgt_hit.astype(jnp.float32)) / TOKENS).astype(jnp.bfloat16)
        grad_hid = jnp.dot(grad_logits, w_out, preferred_element_type=jnp.float32)
        grad_w = grad_w + jnp.dot(grad_logits.T, hid_blk, preferred_element_type=jnp.float32)
        return grad_w, (jnp.sum(log_norm - tgt_logit), grad_hid)

    grad_w, (loss_terms, grad_hid) = lax.scan(scan_step, jnp.zeros((VOCAB_SIZE, MODEL_DIM), jnp.float32), (hid_blocks, tgt_blocks))
    loss_val = (jnp.sum(loss_terms) / TOKENS).reshape(1)
    return loss_val, grad_hid.reshape(TOKENS, MODEL_DIM), grad_w
```

```python
import functools

import jax
import jax.numpy as jnp
from jax import lax
from jax.experimental import pallas as pl
from jax.experimental.pallas import tpu as pltpu
from jax.sharding import PartitionSpec as P

MESH = pl.DeviceIdType.MESH
F32 = jnp.float32
BF16 = jnp.bfloat16

LANES = ((0, 256), (256, 512), (512, 640))
ORDERS = (("x", "y", "z"), ("y", "z", "x"), ("z", "x", "y"))


def remote(src, dst, send, recv, dev):
    return pltpu.make_async_remote_copy(
        src_ref=src, dst_ref=dst, send_sem=send, recv_sem=recv, device_id={"fsdp": dev}, device_id_type=MESH
    )


def greet(peers):
    barrier = pltpu.get_barrier_semaphore()
    for p in peers:
        pl.semaphore_signal(barrier, inc=1, device_id={"fsdp": p}, device_id_type=MESH)
    pl.semaphore_wait(barrier, len(peers))


def merge(parts):
    top = functools.reduce(jnp.maximum, [p[0] for p in parts])
    total = functools.reduce(jnp.add, [p[1] * jnp.exp(p[0] - top) for p in parts])
    target = functools.reduce(jnp.add, [p[2] for p in parts])
    return top, total, target


def stats_kernel(st_ref, out_ref, a_buf, b_buf, o_buf, s1, r1, s2, r2, s3, r3):
    me = lax.axis_index("fsdp")
    g, q = me % 8, me // 8
    row = [q * 8 + (g + k) % 8 for k in range(1, 8)]
    plane = [((q + k) % 16) * 8 + g for k in range(1, 16)]
    greet(row + plane)
    c1 = [remote(st_ref.at[(g + k) % 8], a_buf.at[k - 1], s1.at[k - 1], r1.at[k - 1], row[k - 1]) for k in range(1, 8)]
    for c in c1:
        c.start()
    for c in c1:
        c.wait()
    part = merge([[st_ref[g, i] for i in range(3)]] + [[a_buf[k, i] for i in range(3)] for k in range(7)])
    for i in range(3):
        b_buf[q, i] = part[i]
    c2 = [remote(b_buf.at[q], b_buf.at[q], s2.at[k - 1], r2.at[k - 1], plane[k - 1]) for k in range(1, 16)]
    for c in c2:
        c.start()
    for c in c2:
        c.wait()
    top, total, target = merge([[b_buf[k, i] for i in range(3)] for k in range(16)])
    lse = top + jnp.log(total)
    o_buf[g, 0] = lse
    o_buf[g, 1] = lse - target
    c3 = [remote(o_buf.at[g], o_buf.at[g], s3.at[k - 1], r3.at[k - 1], row[k - 1]) for k in range(1, 8)]
    for c in c3:
        c.start()
    for c in c3:
        c.wait()
    out_ref[...] = o_buf[...]


def stats_exchange(stats):
    dma = pltpu.SemaphoreType.DMA
    return pl.pallas_call(
        stats_kernel,
        out_shape=jax.ShapeDtypeStruct((8, 2, 8, 128), F32),
        in_specs=[pl.BlockSpec(memory_space=pltpu.VMEM)],
        out_specs=pl.BlockSpec(memory_space=pltpu.VMEM),
        scratch_shapes=[
            pltpu.VMEM((7, 3, 8, 128), F32),
            pltpu.VMEM((16, 3, 8, 128), F32),
            pltpu.VMEM((8, 2, 8, 128), F32),
            dma((7,)), dma((7,)), dma((15,)), dma((15,)), dma((7,)), dma((7,)),
        ],
        compiler_params=pltpu.CompilerParams(collective_id=0, has_side_effects=True),
    )(stats)


class Scatter:
    def __init__(self, units, rows, bufs):
        self.units, self.rows = units, rows
        (self.pbuf, self.r0, self.s0, self.v1, self.s1, self.v2, self.s2, self.v3,
         self.csend, self.crecv, self.send, self.recv) = bufs
        me = lax.axis_index("fsdp")
        self.core = me % 2
        self.xyz = {"x": (me // 2) % 4, "y": (me // 8) % 4, "z": me // 32}
        self.me = me
        self.partner = me + 1 - 2 * self.core

    STRIDE = {"x": 2, "y": 8, "z": 32}

    def near(self, axis, k):
        pos = self.xyz[axis]
        return self.me + ((pos + k) % 4 - pos) * self.STRIDE[axis]

    def peers(self):
        return [self.partner] + [self.near(a, k) for a in "xyz" for k in (1, 2, 3)]

    def axes(self, u, j):
        return ORDERS[(j + u) % 3]

    @staticmethod
    def scratch(units, rows, slots):
        dma = pltpu.SemaphoreType.DMA
        widths = [b - a for a, b in LANES]
        return [
            pltpu.VMEM((slots, 64, 2, rows, 640), F32),
            pltpu.VMEM((units, 64, rows, 640), F32),
            [pltpu.VMEM((slots, 2, 4, 8, rows, w), F32) for w in widths],
            [pltpu.VMEM((units, 6, 8, rows, w), F32) for w in widths],
            [pltpu.VMEM((slots, 2, 4, 2, rows, w), F32) for w in widths],
            [pltpu.VMEM((units, 6, 2, rows, w), F32) for w in widths],
            [pltpu.VMEM((slots, 4, rows, w), F32) for w in widths],
            [pltpu.VMEM((units, 3, rows, w), F32) for w in widths],
            dma((units,)), dma((units,)), dma((units, 3, 15)), dma((units, 3, 15)),
        ]

    def core_copy(self, u, slot):
        return remote(self.pbuf.at[slot, :, 1 - self.core], self.r0.at[u], self.csend.at[u], self.crecv.at[u], self.partner)

    def ring_copy(self, u, j, slot, level, kind):
        src, dst = ((self.s0, self.v1), (self.s1, self.v2))[level]
        axis = self.axes(u, j)[level]
        pos = self.xyz[axis]
        up, down = self.near(axis, 1), self.near(axis, 3)
        half, owner, dev = (
            (0, pos + 2, up), (1, pos + 2, down),
            (1, pos + 1, up), (0, pos + 3, down),
            (0, pos + 1, up), (1, pos + 3, down),
        )[kind]
        n = level * 6 + kind
        return remote(src[j].at[slot, half, owner % 4], dst[j].at[u, kind], self.send.at[u, j, n], self.recv.at[u, j, n], dev)

    def last_copy(self, u, j, slot, k):
        axis = self.axes(u, j)[2]
        owner = (self.xyz[axis] + k) % 4
        n = 11 + k
        return remote(self.s2[j].at[slot, owner], self.v3[j].at[u, k - 1], self.send.at[u, j, n], self.recv.at[u, j, n], self.near(axis, k))

    def start_core(self, u, slot):
        self.core_copy(u, slot).start()

    def spread(self, u, slot):
        c = self.core_copy(u, slot)
        c.wait_recv()

        def body(i, _):
            at = {"z": i // 16, "y": (i // 4) % 4, "x": i % 4}
            for j, (lo, hi) in enumerate(LANES):
                a, b, d = (at[n] for n in self.axes(u, j))
                self.s0[j][slot, d // 2, a, b * 2 + d % 2] = (
                    self.pbuf[slot, i, self.core, :, lo:hi] + self.r0[u, i, :, lo:hi]
                )
            return 0

        lax.fori_loop(0, 64, body, 0, unroll=4)
        c.wait_send()
        for kind in range(4):
            for j in range(3):
                self.ring_copy(u, j, slot, 0, kind).start()

    def relay(self, u, slot, level):
        src, dst = ((self.s0, self.v1), (self.s1, self.v2))[level]
        for kind in range(2):
            for j in range(3):
                axis = self.axes(u, j)[level]
                owner = (self.xyz[axis] + (1, 3)[kind]) % 4
                self.ring_copy(u, j, slot, level, kind).wait_recv()
                src[j][slot, kind, owner] = src[j][slot, kind, owner] + dst[j][u, kind]
                self.ring_copy(u, j, slot, level, 4 + kind).start()

    def settle(self, u, slot, level):
        src, dst = ((self.s0, self.v1), (self.s1, self.v2))[level]
        for j in range(3):
            pos = self.xyz[self.axes(u, j)[level]]
            for kind in range(2, 6):
                self.ring_copy(u, j, slot, level, kind).wait_recv()
            for half in range(2):
                total = (src[j][slot, half, pos] + dst[j][u, 4 + half]) + dst[j][u, 3 - half]
                if level == 0:
                    for b in range(4):
                        self.s1[j][slot, half, b] = total[b * 2 : b * 2 + 2]
                else:
                    self.s2[j][slot, half * 2 : half * 2 + 2] = total
            if level == 0:
                for kind in range(4):
                    self.ring_copy(u, j, slot, 1, kind).start()
            else:
                for k in range(1, 4):
                    self.last_copy(u, j, slot, k).start()
        for j in range(3):
            for kind in range(6):
                self.ring_copy(u, j, slot, level, kind).wait_send()

    def finish(self, u, slot, out_ref):
        for j, (lo, hi) in enumerate(LANES):
            for k in range(1, 4):
                self.last_copy(u, j, slot, k).wait_recv()
            pos = self.xyz[self.axes(u, j)[2]]
            total = (self.s2[j][slot, pos] + self.v3[j][u, 0]) + (self.v3[j][u, 1] + self.v3[j][u, 2])
            out_ref[u * self.rows : (u + 1) * self.rows, lo:hi] = total
        for j in range(3):
            for k in range(1, 4):
                self.last_copy(u, j, slot, k).wait_send()


UNITS, ROWS, SLOTS = 4, 16, 2


def scatter_kernel(part_ref, out_ref, load_sem, *bufs):
    rs = Scatter(UNITS, ROWS, bufs)
    greet(rs.peers())

    def load(u):
        return pltpu.make_async_copy(part_ref.at[:, :, u], rs.pbuf.at[u % SLOTS], load_sem.at[u])

    stages = [
        lambda u, s: load(u).start(),
        lambda u, s: (load(u).wait(), rs.start_core(u, s)),
        rs.spread,
        lambda u, s: rs.relay(u, s, 0),
        lambda u, s: rs.settle(u, s, 0),
        lambda u, s: rs.relay(u, s, 1),
        lambda u, s: rs.settle(u, s, 1),
        lambda u, s: rs.finish(u, s, out_ref),
    ]
    for t in range(UNITS + len(stages) - 1):
        for n in reversed(range(len(stages))):
            if 0 <= t - n < UNITS:
                stages[n](t - n, (t - n) % SLOTS)


def scatter(part):
    return pl.pallas_call(
        scatter_kernel,
        out_shape=jax.ShapeDtypeStruct((64, 640), F32),
        in_specs=[pl.BlockSpec(memory_space=pl.ANY)],
        out_specs=pl.BlockSpec(memory_space=pltpu.VMEM),
        scratch_shapes=[pltpu.SemaphoreType.DMA((UNITS,))] + Scatter.scratch(UNITS, ROWS, SLOTS),
        compiler_params=pltpu.CompilerParams(collective_id=1, has_side_effects=True, vmem_limit_bytes=60 * 2**20),
    )(part.reshape(64, 2, UNITS, ROWS, 640))


def solution(mesh):
    def local_step(hidden, targets, w_blk):
        tokens, vocab = hidden.shape[0], w_blk.shape[0]
        start = lax.axis_index("fsdp") * vocab
        logits = jnp.einsum("td,vd->tv", hidden, w_blk, preferred_element_type=F32)
        top = jnp.max(logits, axis=1, keepdims=True)
        hit = (lax.broadcasted_iota(jnp.int32, (1, vocab), 1) + start) == targets[:, None]
        total = jnp.sum(jnp.exp(logits - top), axis=1)
        target = jnp.sum(jnp.where(hit, logits, 0.0), axis=1)
        stats = jnp.stack([top[:, 0], total, target]).reshape(3, 8, 8, 128).transpose(1, 0, 2, 3)
        got = stats_exchange(stats)
        lse = got[:, 0].reshape(tokens, 1)
        loss = (jnp.sum(got[:, 1]) / tokens).reshape(1)
        dz = ((jnp.exp(logits - lse) - hit.astype(F32)) / tokens).astype(BF16)
        part = jnp.einsum("tv,vd->td", dz, w_blk, preferred_element_type=F32)
        grad_hid = scatter(part)
        grad_w = jnp.einsum("tv,td->vd", dz, hidden, preferred_element_type=F32)
        return loss, grad_hid, grad_w

    return jax.shard_map(
        local_step,
        mesh=mesh,
        in_specs=(P("data", None), P("data"), P("fsdp", None)),
        out_specs=(P("data"), P(("data", "fsdp"), None), P(("data", "fsdp"), None)),
        check_vma=False,
    )
```

```python
import functools

import jax
import jax.numpy as jnp
from jax import lax
from jax.experimental import pallas as pl
from jax.experimental.pallas import tpu as pltpu
from jax.sharding import PartitionSpec as P

MESH = pl.DeviceIdType.MESH
F32 = jnp.float32
BF16 = jnp.bfloat16
COMM = True

TOKENS, DIM, VOCAB = 8192, 640, 2048
UNITS, ROWS = 8, 8
SIZE = TOKENS // UNITS
BLOCK = 256
SLOTS = 4
LANES = ((0, 256), (256, 512), (512, 640))
STRIDES = (2, 8, 32)


def dot(a, b, ca, cb):
    return lax.dot_general(a, b, (((ca,), (cb,)), ((), ())), preferred_element_type=F32)


def pick(n, values):
    return jnp.where(n == 0, values[0], jnp.where(n == 1, values[1], values[2]))


def remote(src, dst, send, recv, dev):
    return pltpu.make_async_remote_copy(
        src_ref=src, dst_ref=dst, send_sem=send, recv_sem=recv, device_id={"fsdp": dev}, device_id_type=MESH
    )


def merge(parts):
    top = functools.reduce(jnp.maximum, [p[0:1] for p in parts])
    total = functools.reduce(jnp.add, [p[1:2] * jnp.exp(p[0:1] - top) for p in parts])
    return top, total


class Place:
    def __init__(self):
        self.me = me = lax.axis_index("fsdp") if COMM else 5
        self.g, self.q = me % 8, me // 8
        self.core = me % 2
        self.partner = me + 1 - 2 * self.core
        self.pos = ((me // 2) % 4, (me // 8) % 4, me // 32)
        self.row = [self.q * 8 + (self.g + k) % 8 for k in range(1, 8)]
        self.plane = [((self.q + k) % 16) * 8 + self.g for k in range(1, 16)]

    def near(self, axis, k):
        pos = pick(axis, self.pos)
        return self.me + ((pos + k) % 4 - pos) * pick(axis, STRIDES)

    def greet(self):
        barrier = pltpu.get_barrier_semaphore()
        for p in self.row + self.plane:
            pl.semaphore_signal(barrier, inc=1, device_id={"fsdp": p}, device_id_type=MESH)
        pl.semaphore_wait(barrier, 22)


class Stats:
    def __init__(self, place, bufs):
        self.p = place
        self.own, self.a, self.b, self.lse, self.send, self.recv = bufs

    @staticmethod
    def scratch():
        dma = pltpu.SemaphoreType.DMA
        return [
            pltpu.VMEM((SLOTS, 8, 2, 128), F32),
            pltpu.VMEM((SLOTS, 7, 2, 128), F32),
            pltpu.VMEM((SLOTS, 16, 2, 128), F32),
            pltpu.VMEM((SLOTS, 8, 1, 128), F32),
            dma((SLOTS, 29)),
            dma((SLOTS, 29)),
        ]

    def first(self, s):
        return [
            remote(self.own.at[s, (self.p.g + k) % 8], self.a.at[s, k - 1], self.send.at[s, k - 1], self.recv.at[s, k - 1], self.p.row[k - 1])
            for k in range(1, 8)
        ]

    def second(self, s):
        mine = self.b.at[s, self.p.q]
        return [
            remote(mine, mine, self.send.at[s, 6 + k], self.recv.at[s, 6 + k], self.p.plane[k - 1])
            for k in range(1, 16)
        ]

    def third(self, s):
        mine = self.lse.at[s, self.p.g]
        return [
            remote(mine, mine, self.send.at[s, 21 + k], self.recv.at[s, 21 + k], self.p.row[k - 1])
            for k in range(1, 8)
        ]

    def start_first(self, s):
        for c in self.first(s):
            c.start()

    def start_second(self, s):
        for c in self.first(s):
            c.wait()
        top, total = merge([self.own[s, self.p.g]] + [self.a[s, k] for k in range(7)])
        self.b[s, self.p.q] = jnp.concatenate([top, total], axis=0)
        for c in self.second(s):
            c.start()

    def start_third(self, s):
        for c in self.second(s):
            c.wait()
        top, total = merge([self.b[s, k] for k in range(16)])
        self.lse[s, self.p.g] = top + jnp.log(total)
        for c in self.third(s):
            c.start()

    def wait_third(self, s):
        for c in self.third(s):
            c.wait()


class Scatter:
    def __init__(self, place, bufs):
        self.p = place
        (self.pbuf, self.r0, self.s0, self.v1, self.s1, self.v2, self.s2, self.v3,
         self.csend, self.crecv, self.send, self.recv) = bufs

    @staticmethod
    def scratch():
        dma = pltpu.SemaphoreType.DMA
        widths = [b - a for a, b in LANES]
        return [
            pltpu.VMEM((64, 2, ROWS, DIM), F32),
            pltpu.VMEM((2, 64, ROWS, DIM), F32),
            [pltpu.VMEM((2, 2, 4, 8, ROWS, w), F32) for w in widths],
            [pltpu.VMEM((SLOTS, 6, 8, ROWS, w), F32) for w in widths],
            [pltpu.VMEM((2, 2, 4, 2, ROWS, w), F32) for w in widths],
            [pltpu.VMEM((SLOTS, 6, 2, ROWS, w), F32) for w in widths],
            [pltpu.VMEM((2, 4, ROWS, w), F32) for w in widths],
            [pltpu.VMEM((SLOTS, 3, ROWS, w), F32) for w in widths],
            dma((2,)), dma((2,)), dma((SLOTS, 3, 15)), dma((SLOTS, 3, 15)),
        ]

    def axis(self, u, j, level):
        return (u + j + level) % 3

    def bufs(self, level):
        return ((self.s0, self.v1), (self.s1, self.v2))[level]

    def core_copy(self, u):
        s = u % 2
        return remote(self.pbuf.at[:, 1 - self.p.core], self.r0.at[s], self.csend.at[s], self.crecv.at[s], self.p.partner)

    def ring_copy(self, u, j, level, kind):
        src, dst = self.bufs(level)
        axis = self.axis(u, j, level)
        pos = pick(axis, self.p.pos)
        half, step, way = ((0, 2, 1), (1, 2, 3), (1, 1, 1), (0, 3, 3), (0, 1, 1), (1, 3, 3))[kind]
        n, s = level * 6 + kind, u % SLOTS
        return remote(
            src[j].at[u % 2, half, (pos + step) % 4], dst[j].at[s, kind], self.send.at[s, j, n], self.recv.at[s, j, n],
            self.p.near(axis, way),
        )

    def last_copy(self, u, j, k):
        axis = self.axis(u, j, 2)
        owner = (pick(axis, self.p.pos) + k) % 4
        n, s = 11 + k, u % SLOTS
        return remote(
            self.s2[j].at[u % 2, owner], self.v3[j].at[s, k - 1], self.send.at[s, j, n], self.recv.at[s, j, n],
            self.p.near(axis, k),
        )

    def start_core(self, u):
        self.core_copy(u).start()

    def spread(self, u):
        c = self.core_copy(u)
        c.wait_recv()
        s = u % 2

        def body(i, _):
            at = (i % 4, (i // 4) % 4, i // 16)
            for j, (lo, hi) in enumerate(LANES):
                a, b, d = (pick(self.axis(u, j, n), at) for n in range(3))
                self.s0[j][s, d // 2, a, b * 2 + d % 2] = (
                    self.pbuf[i, self.p.core, :, lo:hi] + self.r0[s, i, :, lo:hi]
                )
            return 0

        lax.fori_loop(0, 64, body, 0, unroll=4)
        c.wait_send()
        for kind in range(4):
            for j in range(3):
                self.ring_copy(u, j, 0, kind).start()

    def relay(self, u, level):
        src, dst = self.bufs(level)
        for kind in range(2):
            for j in range(3):
                owner = (pick(self.axis(u, j, level), self.p.pos) + (1, 3)[kind]) % 4
                self.ring_copy(u, j, level, kind).wait_recv()
                src[j][u % 2, kind, owner] = src[j][u % 2, kind, owner] + dst[j][u % SLOTS, kind]
                self.ring_copy(u, j, level, 4 + kind).start()

    def settle(self, u, level):
        src, dst = self.bufs(level)
        s, v = u % 2, u % SLOTS
        for j in range(3):
            pos = pick(self.axis(u, j, level), self.p.pos)
            for kind in range(2, 6):
                self.ring_copy(u, j, level, kind).wait_recv()
            for half in range(2):
                total = (src[j][s, half, pos] + dst[j][v, 4 + half]) + dst[j][v, 3 - half]
                if level == 0:
                    for b in range(4):
                        self.s1[j][s, half, b] = total[b * 2 : b * 2 + 2]
                else:
                    self.s2[j][s, half * 2 : half * 2 + 2] = total
            if level == 0:
                for kind in range(4):
                    self.ring_copy(u, j, 1, kind).start()
            else:
                for k in range(1, 4):
                    self.last_copy(u, j, k).start()
        for j in range(3):
            for kind in range(6):
                self.ring_copy(u, j, level, kind).wait_send()

    def finish(self, u, out_ref):
        v = u % SLOTS
        for j, (lo, hi) in enumerate(LANES):
            for k in range(1, 4):
                self.last_copy(u, j, k).wait_recv()
            pos = pick(self.axis(u, j, 2), self.p.pos)
            total = (self.s2[j][u % 2, pos] + self.v3[j][v, 0]) + (self.v3[j][v, 1] + self.v3[j][v, 2])
            out_ref[pl.ds(pl.multiple_of(u * ROWS, ROWS), ROWS), lo:hi] = total
        for j in range(3):
            for k in range(1, 4):
                self.last_copy(u, j, k).wait_send()


def main_kernel(h_ref, w_ref, tgt_ref, loss_ref, dh_ref, dw_ref, hb, wb, zb, dzb, acc, lse_col, tgt_col, lost,
                la, lb, h_sem, w_sem, out_sem, lsend, lrecv, *bufs):
    place = Place()
    stats = Stats(place, bufs[:6])
    rs = Scatter(place, bufs[6:])
    start = place.me * VOCAB

    def load_h(t):
        s = t % 4
        return pltpu.make_async_copy(h_ref.at[:, t], hb.at[s], h_sem.at[s])

    load_w = pltpu.make_async_copy(w_ref, wb, w_sem)
    load_w.start()
    load_h(0).start()
    acc[...] = jnp.zeros_like(acc)
    lost[...] = jnp.zeros_like(lost)
    if COMM:
        place.greet()
    load_w.wait()

    lane = lax.broadcasted_iota(jnp.int32, (64, 128), 1)

    def local_stats(t, rb):
        z, s = t % 3, t % SLOTS
        for half in range(2):
            cols = []
            for part in range(2):
                r = rb * BLOCK + half * 128 + part * 64
                rows = slice(r, r + 64)
                top = functools.reduce(jnp.maximum, [zb[z, rows, c : c + 128] for c in range(0, VOCAB, 128)])
                top = jnp.max(top, axis=1, keepdims=True)
                total = functools.reduce(jnp.add, [jnp.exp(zb[z, rows, c : c + 128] - top) for c in range(0, VOCAB, 128)])
                total = jnp.sum(total, axis=1, keepdims=True)
                cols.append(jnp.where(lane == 0, top, total))
            packed = jnp.concatenate(cols, axis=0).T
            stats.own[s, rb * 2 + half] = packed[0:2]

    def logits(t):
        h = hb.at[t % 4]
        for rb in range(SIZE // BLOCK):
            rows = slice(rb * BLOCK, (rb + 1) * BLOCK)
            d = BLOCK // ROWS
            hv = h[rb * d : (rb + 1) * d].reshape(BLOCK, DIM)
            zb[t % 3, rows, :] = dot(hv, wb[...], 1, 1)
            if rb:
                local_stats(t, rb - 1)
        local_stats(t, SIZE // BLOCK - 1)

    def columns(u):
        for g in range(8):
            rows = slice(g * 128, (g + 1) * 128)
            lse_col[rows, :] = jnp.broadcast_to(stats.lse[u % SLOTS, g], (128, 128)).T
            tgt_col[rows, :] = jnp.broadcast_to(tgt_ref[u, g : g + 1, :] - start, (128, 128)).T

    def grad_logits(u, rb):
        z = u % 3
        for part in range(BLOCK // 64):
            r = rb * BLOCK + part * 64
            rows = slice(r, r + 64)
            lse, tgt = lse_col[rows, :], tgt_col[rows, :]
            found = []
            for c in range(0, VOCAB, 128):
                x = zb[z, rows, c : c + 128] - lse
                hit = (lane + c) == tgt
                found.append(jnp.where(hit, x, 0.0))
                dzb[rows, c : c + 128] = ((jnp.exp(x) - jnp.where(hit, 1.0, 0.0)) * (1.0 / TOKENS)).astype(BF16)
            lost[...] += functools.reduce(jnp.add, found)

    def grad_hidden(u):
        n = SIZE // BLOCK
        d = BLOCK // ROWS // 2
        grad_logits(u, 0)
        for rb in range(n):
            rows = slice(rb * BLOCK, (rb + 1) * BLOCK)
            rs.pbuf[rb * d : (rb + 1) * d] = dot(dzb[rows, :], wb[...], 1, 0).reshape(d, 2, ROWS, DIM)
            if rb + 1 < n:
                grad_logits(u, rb + 1)

    def grad_weight(u):
        acc[...] += dot(hb[u % 4].reshape(SIZE, DIM), dzb[...], 0, 0)

    def step(t, _):
        u = t - 2
        old, older = t - 3, t - 4

        @pl.when(t + 1 < UNITS)
        def _():
            load_h(t + 1).start()

        @pl.when(t < UNITS)
        def _():
            load_h(t).wait()
            logits(t)
            if COMM:
                stats.start_first(t % SLOTS)

        if COMM:
            @pl.when(old >= 0)
            def _():
                rs.relay(old, 0)

            @pl.when(older >= 0)
            def _():
                rs.settle(older, 1)

        @pl.when(u >= 0)
        def _():
            if COMM:
                stats.wait_third(u % SLOTS)
            columns(u)
            grad_hidden(u)
            if COMM:
                rs.start_core(u)

        if COMM:
            @pl.when((t >= 1) & (t <= UNITS))
            def _():
                stats.start_third((t - 1) % SLOTS)

            @pl.when(old >= 0)
            def _():
                rs.settle(old, 0)

            @pl.when(older >= 0)
            def _():
                rs.finish(older, dh_ref)

        @pl.when(u >= 0)
        def _():
            grad_weight(u)

        if COMM:
            @pl.when(old >= 0)
            def _():
                rs.relay(old, 1)

            @pl.when(u >= 0)
            def _():
                rs.spread(u)

            @pl.when(t < UNITS)
            def _():
                stats.start_second(t % SLOTS)

        return 0

    lax.fori_loop(0, UNITS + 2, step, 0)
    out = pltpu.make_async_copy(acc, dw_ref, out_sem)
    out.start()
    mine = jnp.sum(lost[...], axis=0, keepdims=True)
    if not COMM:
        loss_ref[...] = mine
        out.wait()
        return
    last = UNITS - 1
    la[place.g] = mine
    row = [remote(la.at[place.g], la.at[place.g], lsend.at[k - 1], lrecv.at[k - 1], place.row[k - 1]) for k in range(1, 8)]
    plane = [remote(lb.at[place.q], lb.at[place.q], lsend.at[6 + k], lrecv.at[6 + k], place.plane[k - 1]) for k in range(1, 16)]
    for c in row:
        c.start()
    rs.relay(last, 0)
    rs.settle(last - 1, 1)
    rs.settle(last, 0)
    for c in row:
        c.wait()
    lb[place.q] = functools.reduce(jnp.add, [la[k] for k in range(8)])
    for c in plane:
        c.start()
    rs.finish(last - 1, dh_ref)
    rs.relay(last, 1)
    rs.settle(last, 1)
    for c in plane:
        c.wait()
    loss_ref[...] = functools.reduce(jnp.add, [lb[k] for k in range(16)])
    rs.finish(last, dh_ref)
    out.wait()


def fused(hidden, targets, w_blk):
    dma = pltpu.SemaphoreType.DMA
    any_spec, vmem = pl.BlockSpec(memory_space=pl.ANY), pl.BlockSpec(memory_space=pltpu.VMEM)
    return pl.pallas_call(
        main_kernel,
        out_shape=(
            jax.ShapeDtypeStruct((1, 128), F32),
            jax.ShapeDtypeStruct((64, DIM), F32),
            jax.ShapeDtypeStruct((DIM, VOCAB), F32),
        ),
        in_specs=[any_spec, any_spec, vmem],
        out_specs=(vmem, vmem, any_spec),
        scratch_shapes=[
            pltpu.VMEM((4, 128, ROWS, DIM), BF16),
            pltpu.VMEM((VOCAB, DIM), BF16),
            pltpu.VMEM((3, SIZE, VOCAB), F32),
            pltpu.VMEM((SIZE, VOCAB), BF16),
            pltpu.VMEM((DIM, VOCAB), F32),
            pltpu.VMEM((SIZE, 128), F32),
            pltpu.VMEM((SIZE, 128), jnp.int32),
            pltpu.VMEM((64, 128), F32),
            pltpu.VMEM((8, 1, 128), F32),
            pltpu.VMEM((16, 1, 128), F32),
            dma((4,)), dma, dma, dma((22,)), dma((22,)),
        ] + Stats.scratch() + Scatter.scratch(),
        compiler_params=pltpu.CompilerParams(
            vmem_limit_bytes=67043328, **(dict(collective_id=0, has_side_effects=True) if COMM else {})
        ),
    )(hidden, w_blk, targets)


def prepare(hidden, targets):
    h = hidden.reshape(128, UNITS, ROWS, DIM)
    t = targets.reshape(128, UNITS, ROWS).transpose(1, 0, 2).reshape(UNITS, 8, 128)
    return h, t


def solution(mesh):
    def local_step(hidden, targets, w_blk):
        h, t = prepare(hidden, targets)
        lost, grad_hid, grad_w = fused(h, t, w_blk)
        loss = (-jnp.sum(lost) / hidden.shape[0]).reshape(1)
        return loss, grad_hid, grad_w.T

    return jax.shard_map(
        local_step,
        mesh=mesh,
        in_specs=(P("data", None), P("data"), P("fsdp", None)),
        out_specs=(P("data"), P(("data", "fsdp"), None), P(("data", "fsdp"), None)),
        check_vma=False,
    )
```

```python
import functools

import jax
import jax.numpy as jnp
from jax import lax
from jax.experimental import pallas as pl
from jax.experimental.pallas import tpu as pltpu
from jax.sharding import PartitionSpec as P

MESH = pl.DeviceIdType.MESH
F32 = jnp.float32
BF16 = jnp.bfloat16
COMM = True

TOKENS, DIM, VOCAB = 8192, 640, 2048
UNITS, ROWS = 8, 8
SIZE = TOKENS // UNITS
BLOCK = 256
FEW = 16
SLOTS = 4
LANES = ((0, 256), (256, 512), (512, 640))
STRIDES = (2, 8, 32)


def mod(a, n):
    return a % n if isinstance(a, int) else lax.rem(a, jnp.int32(n))


def div(a, n):
    return a // n if isinstance(a, int) else lax.div(a, jnp.int32(n))


def dot(a, b, ca, cb):
    return lax.dot_general(a, b, (((ca,), (cb,)), ((), ())), preferred_element_type=F32)


def pick(n, values):
    return jnp.where(n == 0, values[0], jnp.where(n == 1, values[1], values[2]))


def remote(src, dst, send, recv, dev):
    return pltpu.make_async_remote_copy(
        src_ref=src, dst_ref=dst, send_sem=send, recv_sem=recv, device_id=(0, dev), device_id_type=MESH
    )


def merge(parts):
    top = functools.reduce(jnp.maximum, [p[0] for p in parts])
    total = functools.reduce(jnp.add, [p[1] * jnp.exp(p[0] - top) for p in parts])
    return top, total


class Place:
    def __init__(self, me):
        self.me = me
        self.g, self.q = mod(me, 8), div(me, 8)
        self.core = mod(me, 2)
        self.partner = me + 1 - 2 * self.core
        self.pos = (mod(div(me, 2), 4), mod(div(me, 8), 4), div(me, 32))
        self.row = [self.q * 8 + mod(self.g + k, 8) for k in range(1, 8)]
        self.plane = [mod(self.q + k, 16) * 8 + self.g for k in range(1, 16)]

    def along(self, axis):
        pos, stride = pick(axis, self.pos), pick(axis, STRIDES)
        at = [pos] + [mod(pos + k, 4) for k in (1, 2, 3)]
        return at, [self.me + (p - pos) * stride for p in at]

    def greet(self):
        barrier = pltpu.get_barrier_semaphore()
        for p in self.row + self.plane:
            pl.semaphore_signal(barrier, inc=1, device_id=(0, p), device_id_type=MESH)
        return barrier


class Stats:
    def __init__(self, place, bufs):
        self.p = place
        self.a, self.b, self.send, self.recv = bufs

    @staticmethod
    def scratch():
        dma = pltpu.SemaphoreType.DMA
        return [
            pltpu.VMEM((SLOTS, 8, 2, 8, 128), F32),
            pltpu.VMEM((SLOTS, 16, 2, 8, 128), F32),
            dma((SLOTS, 22)),
            dma((SLOTS, 22)),
        ]

    def first(self, t):
        s = mod(t, SLOTS)
        mine = self.a.at[s, self.p.g]
        return [remote(mine, mine, self.send.at[s, k], self.recv.at[s, k], self.p.row[k]) for k in range(7)]

    def second(self, t):
        s = mod(t, SLOTS)
        mine = self.b.at[s, self.p.q]
        return [remote(mine, mine, self.send.at[s, 7 + k], self.recv.at[s, 7 + k], self.p.plane[k]) for k in range(15)]

    def start_first(self, t):
        for c in self.first(t):
            c.start()

    def start_second(self, t):
        for c in self.first(t):
            c.wait()
        s = mod(t, SLOTS)
        self.b[s, self.p.q, 0], self.b[s, self.p.q, 1] = merge([self.a[s, k] for k in range(8)])
        for c in self.second(t):
            c.start()

    def wait_second(self, t):
        for c in self.second(t):
            c.wait()

    def lse(self, t):
        top, total = merge([self.b[mod(t, SLOTS), k] for k in range(16)])
        return top + jnp.log(total)


class Scatter:
    def __init__(self, place, bufs):
        self.p = place
        (self.pbuf, self.r0, self.s0, self.v1, self.s1, self.v2, self.s2, self.v3,
         self.csend, self.crecv, self.send, self.recv) = bufs

    @staticmethod
    def scratch():
        dma = pltpu.SemaphoreType.DMA
        widths = [b - a for a, b in LANES]
        return [
            pltpu.VMEM((64, 2, ROWS, DIM), F32),
            pltpu.VMEM((2, 64, ROWS, DIM), F32),
            [pltpu.VMEM((2, 64, ROWS, w), F32) for w in widths],
            [pltpu.VMEM((SLOTS, 6, 8, ROWS, w), F32) for w in widths],
            [pltpu.VMEM((2, 16, ROWS, w), F32) for w in widths],
            [pltpu.VMEM((SLOTS, 6, 2, ROWS, w), F32) for w in widths],
            [pltpu.VMEM((2, 4, ROWS, w), F32) for w in widths],
            [pltpu.VMEM((SLOTS, 3, ROWS, w), F32) for w in widths],
            dma((2,)), dma((2,)), dma((SLOTS, 3, 15)), dma((SLOTS, 3, 15)),
        ]

    def line(self, u, j, level):
        return self.p.along(mod(u + j + level, 3))

    def bufs(self, level):
        return ((self.s0, self.v1), (self.s1, self.v2))[level]

    def piece(self, level, half, owner):
        n = (8, 2)[level]
        return pl.ds((half * 4 + owner) * n, n)

    def core_copy(self, u):
        s = mod(u, 2)
        return remote(self.pbuf.at[:, 1 - self.p.core], self.r0.at[s], self.csend.at[s], self.crecv.at[s], self.p.partner)

    def ring_copies(self, u, j, level, kinds, line):
        src, dst = self.bufs(level)
        at, dev = line
        s, v = mod(u, 2), mod(u, SLOTS)
        copies = []
        for kind in kinds:
            half, step, way = ((0, 2, 1), (1, 2, 3), (1, 1, 1), (0, 3, 3), (0, 1, 1), (1, 3, 3))[kind]
            n = level * 6 + kind
            copies.append(remote(
                src[j].at[s, self.piece(level, half, at[step])], dst[j].at[v, kind], self.send.at[v, j, n],
                self.recv.at[v, j, n], dev[way],
            ))
        return copies

    def last_copies(self, u, j, line):
        at, dev = line
        s, v = mod(u, 2), mod(u, SLOTS)
        return [
            remote(self.s2[j].at[s, at[k]], self.v3[j].at[v, k - 1], self.send.at[v, j, 11 + k], self.recv.at[v, j, 11 + k], dev[k])
            for k in (1, 2, 3)
        ]

    def start_core(self, u):
        self.core_copy(u).start()

    def spread(self, u):
        c = self.core_copy(u)
        c.wait_recv()
        s = mod(u, 2)
        roles = [[mod(n + 3 * UNITS - u - j, 3) for n in range(3)] for j in range(3)]
        at = [[[pick(roles[j][n], (8 * v, 2 * v, v // 2 * 32 + v % 2)) for v in range(4)] for n in range(2)] for j in range(3)]

        def body(z, _):
            last = (8 * z, 2 * z, div(z, 2) * 32 + mod(z, 2))
            for j, (lo, hi) in enumerate(LANES):
                base = pick(roles[j][2], last)
                for i in range(16):
                    n = base + (at[j][0][i % 4] + at[j][1][i // 4])
                    self.s0[j][s, n] = self.pbuf[z * 16 + i, self.p.core, :, lo:hi] + self.r0[s, z * 16 + i, :, lo:hi]
            return 0

        lax.fori_loop(0, 4, body, 0)
        for j in range(3):
            for copy in self.ring_copies(u, j, 0, range(4), self.line(u, j, 0)):
                copy.start()
        c.wait_send()

    def relay(self, u, level):
        src, dst = self.bufs(level)
        s, v = mod(u, 2), mod(u, SLOTS)
        for j in range(3):
            line = self.line(u, j, level)
            far = self.ring_copies(u, j, level, range(2), line)
            on = self.ring_copies(u, j, level, range(4, 6), line)
            for kind in range(2):
                blocks = self.piece(level, kind, line[0][(1, 3)[kind]])
                far[kind].wait_recv()
                src[j][s, blocks] = src[j][s, blocks] + dst[j][v, kind]
                on[kind].start()

    def settle(self, u, level):
        src, dst = self.bufs(level)
        s, v = mod(u, 2), mod(u, SLOTS)
        sent = []
        for j in range(3):
            line = self.line(u, j, level)
            copies = self.ring_copies(u, j, level, range(6), line)
            sent += copies
            for copy in copies[2:]:
                copy.wait_recv()
            for half in range(2):
                total = (src[j][s, self.piece(level, half, line[0][0])] + dst[j][v, 4 + half]) + dst[j][v, 3 - half]
                if level == 0:
                    self.s1[j][s, half * 8 : half * 8 + 8] = total
                else:
                    self.s2[j][s, half * 2 : half * 2 + 2] = total
            after = self.line(u, j, level + 1)
            for copy in self.last_copies(u, j, after) if level else self.ring_copies(u, j, 1, range(4), after):
                copy.start()
        for copy in sent:
            copy.wait_send()

    def finish(self, u, out_ref):
        s, v = mod(u, 2), mod(u, SLOTS)
        for j, (lo, hi) in enumerate(LANES):
            line = self.line(u, j, 2)
            copies = self.last_copies(u, j, line)
            for copy in copies:
                copy.wait_recv()
            total = (self.s2[j][s, line[0][0]] + self.v3[j][v, 0]) + (self.v3[j][v, 1] + self.v3[j][v, 2])
            out_ref[pl.ds(pl.multiple_of(u * ROWS, ROWS), ROWS), lo:hi] = total
            for copy in copies:
                copy.wait_send()


def main_kernel(h_ref, w_ref, tgt_ref, loss_ref, dh_ref, dw_ref, hb, wb, zb, dzb, acc, lse_col, tgt_col, lost,
                la, lb, h_sem, w_sem, out_sem, lsend, lrecv, *bufs):
    place = Place(lax.axis_index("fsdp") if COMM else jnp.minimum(tgt_ref[0, 0, 0], 0) + 5)
    stats = Stats(place, bufs[:4])
    rs = Scatter(place, bufs[4:])
    start = place.me * VOCAB
    blocks, quarter = SIZE // BLOCK, VOCAB // 4

    def load_h(t):
        return pltpu.make_async_copy(h_ref.at[:, t], hb.at[mod(t, 4)], h_sem.at[mod(t, 4)])

    load_w = pltpu.make_async_copy(w_ref, wb, w_sem)
    load_w.start()
    load_h(0).start()
    if COMM:
        barrier = place.greet()
    acc[...] = jnp.zeros_like(acc)
    lost[...] = jnp.zeros_like(lost)
    load_w.wait()

    lane = lax.broadcasted_iota(jnp.int32, (FEW, 128), 1)
    column = lax.broadcasted_iota(jnp.int32, (FEW, VOCAB), 1)

    def wide(x):
        return jnp.concatenate([x] * (VOCAB // 128), axis=1)

    def logits(t, rb):
        d = BLOCK // ROWS
        h = hb[mod(t, 4), rb * d : (rb + 1) * d].reshape(BLOCK, DIM)
        zb[mod(t, 3), rb * BLOCK : (rb + 1) * BLOCK, :] = dot(h, wb[...], 1, 1)

    def local_stats(t, n):
        z, s = mod(t, 3), mod(t, SLOTS)
        cols = []
        for r in range(n * 128, n * 128 + 128, FEW):
            x = zb[z, r : r + FEW, :]
            top = jnp.max(x, axis=1, keepdims=True)
            total = jnp.sum(jnp.exp(x - top), axis=1, keepdims=True)
            cols.append(jnp.where(lane == 0, top, total))
        packed = jnp.concatenate(cols, axis=0).T
        for i in range(2):
            stats.a[s, place.g, i, n : n + 1] = packed[i : i + 1]

    def columns(u):
        lse = stats.lse(u)
        for g in range(8):
            rows = slice(g * 128, (g + 1) * 128)
            lse_col[rows, :] = jnp.broadcast_to(lse[g : g + 1], (128, 128)).T
            tgt_col[rows, :] = jnp.broadcast_to(tgt_ref[u, g : g + 1, :] - start, (128, 128)).T

    def grad_logits(u, first, last):
        for r in range(first * 64, last * 64, FEW):
            rows = slice(r, r + FEW)
            x = zb[mod(u, 3), rows, :] - wide(lse_col[rows, :])
            hit = column == wide(tgt_col[rows, :])
            dzb[rows, :] = ((jnp.exp(x) - jnp.where(hit, 1.0, 0.0)) * (1.0 / TOKENS)).astype(BF16)
            found = jnp.where(hit, x, 0.0)
            lost[...] += sum(found[:, c : c + 128] for c in range(0, VOCAB, 128))

    def grad_hidden(rb):
        d = BLOCK // ROWS // 2
        rows = slice(rb * BLOCK, (rb + 1) * BLOCK)
        rs.pbuf[rb * d : (rb + 1) * d] = dot(dzb[rows, :], wb[...], 1, 0).reshape(d, 2, ROWS, DIM)

    def grad_weight(u):
        for lo in range(0, VOCAB, quarter):
            acc[:, lo : lo + quarter] += dot(hb[mod(u, 4)].reshape(SIZE, DIM), dzb[:, lo : lo + quarter], 0, 0)

    def when(cond, f, *args):
        if COMM:
            pl.when(cond)(lambda: f(*args))

    def step(t, _):
        u, old, older = t - 2, t - 3, t - 4
        mix = (t >= 3) & (t < UNITS)
        ending = t >= UNITS
        alone = (t >= 2) & ((t - 3) * (UNITS - 1 - t) < 0)

        @pl.when(t + 1 < UNITS)
        def _():
            load_h(t + 1).start()

        @pl.when(t < UNITS)
        def _():
            load_h(t).wait()

        for rb in range(blocks + 1):
            @pl.when(t < 3)
            def first():
                if rb < blocks:
                    logits(t, rb)
                if rb:
                    local_stats(t, 2 * rb - 2)
                    local_stats(t, 2 * rb - 1)

        if COMM:
            when(t < 3, stats.start_first, t)
            when((t >= 1) & (t < 3), stats.start_second, t - 1)
            when(t >= 2, stats.wait_second, u)
            when(t == UNITS + 1, rs.relay, older, 1)

        @pl.when(mix)
        def mixed_logits():
            logits(t, 0)
            columns(u)
            grad_logits(u, 0, 4)
            for rb in range(1, blocks):
                logits(t, rb)
                local_stats(t, 2 * rb - 2)
                local_stats(t, 2 * rb - 1)
                grad_logits(u, 3 + rb, 4 + rb)

        when(mix & (old >= 0), rs.relay, old, 0)
        when(mix & (older >= 0), rs.settle, older, 1)

        @pl.when(mix)
        def mixed_hidden():
            grad_hidden(0)
            local_stats(t, 6)
            local_stats(t, 7)
            grad_logits(u, 7, 8)

        when(mix, stats.start_first, t)

        @pl.when(alone)
        def alone_logits():
            columns(u)
            grad_logits(u, 0, 4)

        @pl.when(alone)
        def alone_hidden():
            grad_hidden(0)
            grad_logits(u, 4, 8)

        @pl.when(t >= 2)
        def hidden():
            grad_hidden(1)
            grad_logits(u, 8, 12)
            grad_hidden(2)
            grad_logits(u, 12, 16)
            grad_hidden(3)

        when(t >= 2, rs.start_core, u)
        when(ending, rs.relay, old, 0)
        when(ending, rs.settle, older, 1)
        when(mix & (old >= 0), rs.settle, old, 0)
        when(mix & (older >= 0), rs.finish, older, dh_ref)
        pl.when(t >= 2)(lambda: grad_weight(u))
        when(mix & (old >= 0), rs.relay, old, 1)
        when(ending, rs.settle, old, 0)
        when(ending, rs.finish, older, dh_ref)
        when(t >= 2, rs.spread, u)
        when((t >= 2) & (t < UNITS), stats.start_second, t)
        return 0

    if COMM:
        pl.semaphore_wait(barrier, 22)
    lax.fori_loop(0, UNITS + 2, step, 0)

    def to_rows(n):
        z, r = n // 2, n % 2 * quarter
        for i in range(0, quarter, 128):
            zb[z, r + i : r + i + 128, 0:DIM] = acc[:, n * quarter + i : n * quarter + i + 128].T
        put(n).start()

    def put(n):
        z, r = n // 2, n % 2 * quarter
        return pltpu.make_async_copy(
            zb.at[z, pl.ds(r, quarter), pl.ds(0, DIM)], dw_ref.at[pl.ds(n * quarter, quarter)], out_sem.at[n]
        )

    mine = jnp.sum(lost[...], axis=0, keepdims=True)
    if not COMM:
        for n in range(4):
            to_rows(n)
        loss_ref[...] = jnp.sum(mine, axis=1, keepdims=True)
        for n in range(4):
            put(n).wait()
        return
    la[place.g] = mine
    row = [remote(la.at[place.g], la.at[place.g], lsend.at[k], lrecv.at[k], place.row[k]) for k in range(7)]
    plane = [remote(lb.at[place.q], lb.at[place.q], lsend.at[7 + k], lrecv.at[7 + k], place.plane[k]) for k in range(15)]
    for c in row:
        c.start()
    rs.relay(6, 1)
    to_rows(0)
    to_rows(1)
    rs.relay(7, 0)
    to_rows(2)
    for c in row:
        c.wait()
    lb[place.q] = functools.reduce(jnp.add, [la[k] for k in range(8)])
    for c in plane:
        c.start()
    to_rows(3)
    rs.settle(7, 0)
    rs.settle(6, 1)
    rs.relay(7, 1)
    rs.finish(6, dh_ref)
    rs.settle(7, 1)
    for c in plane:
        c.wait()
    total = functools.reduce(jnp.add, [lb[k] for k in range(16)])
    loss_ref[...] = jnp.sum(total, axis=1, keepdims=True) * (-1.0 / TOKENS)
    rs.finish(7, dh_ref)
    for n in range(4):
        put(n).wait()


def fused(hidden, targets, w_blk):
    dma = pltpu.SemaphoreType.DMA
    any_spec, vmem = pl.BlockSpec(memory_space=pl.ANY), pl.BlockSpec(memory_space=pltpu.VMEM)
    return pl.pallas_call(
        main_kernel,
        out_shape=(
            jax.ShapeDtypeStruct((1, 1), F32),
            jax.ShapeDtypeStruct((64, DIM), F32),
            jax.ShapeDtypeStruct((VOCAB, DIM), F32),
        ),
        in_specs=[any_spec, any_spec, vmem],
        out_specs=(vmem, vmem, any_spec),
        scratch_shapes=[
            pltpu.VMEM((4, 128, ROWS, DIM), BF16),
            pltpu.VMEM((VOCAB, DIM), BF16),
            pltpu.VMEM((3, SIZE, VOCAB), F32),
            pltpu.VMEM((SIZE, VOCAB), BF16),
            pltpu.VMEM((DIM, VOCAB), F32),
            pltpu.VMEM((SIZE, 128), F32),
            pltpu.VMEM((SIZE, 128), jnp.int32),
            pltpu.VMEM((FEW, 128), F32),
            pltpu.VMEM((8, 1, 128), F32),
            pltpu.VMEM((16, 1, 128), F32),
            dma((4,)), dma, dma((4,)), dma((22,)), dma((22,)),
        ] + Stats.scratch() + Scatter.scratch(),
        compiler_params=pltpu.CompilerParams(
            vmem_limit_bytes=67043328, **(dict(collective_id=0, has_side_effects=True) if COMM else {})
        ),
    )(hidden, w_blk, targets)


def prepare(hidden, targets):
    h = hidden.reshape(128, UNITS, ROWS, DIM)
    t = targets.reshape(128, UNITS, ROWS).transpose(1, 0, 2).reshape(UNITS, 8, 128)
    return h, t


def solution(mesh):
    def local_step(hidden, targets, w_blk):
        h, t = prepare(hidden, targets)
        loss, grad_hid, grad_w = fused(h, t, w_blk)
        return loss.reshape(1), grad_hid, grad_w

    return jax.shard_map(
        local_step,
        mesh=mesh,
        in_specs=(P("data", None), P("data"), P("fsdp", None)),
        out_specs=(P("data"), P(("data", "fsdp"), None), P(("data", "fsdp"), None)),
        check_vma=False,
    )
```

```python
import functools

import jax
import jax.numpy as jnp
from jax import lax
from jax.experimental import pallas as pl
from jax.experimental.pallas import tpu as pltpu
from jax.sharding import PartitionSpec as P

MESH = pl.DeviceIdType.MESH
F32 = jnp.float32
BF16 = jnp.bfloat16
COMM = True

TOKENS, DIM, VOCAB = 8192, 640, 2048
UNITS, ROWS = 8, 8
SIZE = TOKENS // UNITS
BLOCK = 256
FEW = 16
SLOTS = 4
LANES = ((0, 256), (256, 512), (512, 640))
STRIDES = (2, 8, 32)


def mod(a, n):
    return a % n if isinstance(a, int) else lax.rem(a, jnp.int32(n))


def div(a, n):
    return a // n if isinstance(a, int) else lax.div(a, jnp.int32(n))


def dot(a, b, ca, cb):
    return lax.dot_general(a, b, (((ca,), (cb,)), ((), ())), preferred_element_type=F32)


def pick(n, values):
    return jnp.where(n == 0, values[0], jnp.where(n == 1, values[1], values[2]))


def remote(src, dst, send, recv, dev):
    return pltpu.make_async_remote_copy(
        src_ref=src, dst_ref=dst, send_sem=send, recv_sem=recv, device_id=(0, dev), device_id_type=MESH
    )


def merge(parts):
    top = functools.reduce(jnp.maximum, [p[0] for p in parts])
    total = functools.reduce(jnp.add, [p[1] * jnp.exp(p[0] - top) for p in parts])
    return top, total


class Place:
    def __init__(self, me):
        self.me = me
        self.g, self.q = mod(me, 8), div(me, 8)
        self.core = mod(me, 2)
        self.partner = me + 1 - 2 * self.core
        self.pos = (mod(div(me, 2), 4), mod(div(me, 8), 4), div(me, 32))
        self.row = [self.q * 8 + mod(self.g + k, 8) for k in range(1, 8)]
        self.plane = [mod(self.q + k, 16) * 8 + self.g for k in range(1, 16)]

    def along(self, axis):
        pos, stride = pick(axis, self.pos), pick(axis, STRIDES)
        at = [pos] + [mod(pos + k, 4) for k in (1, 2, 3)]
        return at, [self.me + (p - pos) * stride for p in at]

    def greet(self):
        barrier = pltpu.get_barrier_semaphore()
        for p in self.row + self.plane:
            pl.semaphore_signal(barrier, inc=1, device_id=(0, p), device_id_type=MESH)
        return barrier


class Stats:
    def __init__(self, place, bufs):
        self.p = place
        self.a, self.b, self.send, self.recv = bufs

    @staticmethod
    def scratch():
        dma = pltpu.SemaphoreType.DMA
        return [
            pltpu.VMEM((SLOTS, 8, 2, 8, 128), F32),
            pltpu.VMEM((SLOTS, 16, 2, 8, 128), F32),
            dma((SLOTS, 22)),
            dma((SLOTS, 22)),
        ]

    def first(self, t):
        s = mod(t, SLOTS)
        mine = self.a.at[s, self.p.g]
        return [remote(mine, mine, self.send.at[s, k], self.recv.at[s, k], self.p.row[k]) for k in range(7)]

    def second(self, t):
        s = mod(t, SLOTS)
        mine = self.b.at[s, self.p.q]
        return [remote(mine, mine, self.send.at[s, 7 + k], self.recv.at[s, 7 + k], self.p.plane[k]) for k in range(15)]

    def start_first(self, t):
        for c in self.first(t):
            c.start()

    def start_second(self, t):
        for c in self.first(t):
            c.wait()
        s = mod(t, SLOTS)
        self.b[s, self.p.q, 0], self.b[s, self.p.q, 1] = merge([self.a[s, k] for k in range(8)])
        for c in self.second(t):
            c.start()

    def wait_second(self, t):
        for c in self.second(t):
            c.wait()

    def lse(self, t):
        top, total = merge([self.b[mod(t, SLOTS), k] for k in range(16)])
        return top + jnp.log(total)


class Scatter:
    def __init__(self, place, bufs):
        self.p = place
        (self.pbuf, self.r0, self.s0, self.v1, self.s1, self.v2, self.s2, self.v3,
         self.csend, self.crecv, self.send, self.recv) = bufs

    @staticmethod
    def scratch():
        dma = pltpu.SemaphoreType.DMA
        widths = [b - a for a, b in LANES]
        return [
            pltpu.VMEM((64, 2, ROWS, DIM), F32),
            pltpu.VMEM((2, 64, ROWS, DIM), F32),
            [pltpu.VMEM((2, 64, ROWS, w), F32) for w in widths],
            [pltpu.VMEM((SLOTS, 6, 8, ROWS, w), F32) for w in widths],
            [pltpu.VMEM((2, 16, ROWS, w), F32) for w in widths],
            [pltpu.VMEM((SLOTS, 6, 2, ROWS, w), F32) for w in widths],
            [pltpu.VMEM((2, 4, ROWS, w), F32) for w in widths],
            [pltpu.VMEM((SLOTS, 3, ROWS, w), F32) for w in widths],
            dma((2,)), dma((2,)), dma((SLOTS, 3, 15)), dma((SLOTS, 3, 15)),
        ]

    def line(self, u, j, level):
        return self.p.along(mod(u + j + level, 3))

    def bufs(self, level):
        return ((self.s0, self.v1), (self.s1, self.v2))[level]

    def piece(self, level, half, owner):
        n = (8, 2)[level]
        return pl.ds((half * 4 + owner) * n, n)

    def core_copy(self, u):
        s = mod(u, 2)
        return remote(self.pbuf.at[:, 1 - self.p.core], self.r0.at[s], self.csend.at[s], self.crecv.at[s], self.p.partner)

    def ring_copies(self, u, j, level, kinds, line):
        src, dst = self.bufs(level)
        at, dev = line
        s, v = mod(u, 2), mod(u, SLOTS)
        copies = []
        for kind in kinds:
            half, step, way = ((0, 2, 1), (1, 2, 3), (1, 1, 1), (0, 3, 3), (0, 1, 1), (1, 3, 3))[kind]
            n = level * 6 + kind
            copies.append(remote(
                src[j].at[s, self.piece(level, half, at[step])], dst[j].at[v, kind], self.send.at[v, j, n],
                self.recv.at[v, j, n], dev[way],
            ))
        return copies

    def last_copies(self, u, j, line):
        at, dev = line
        s, v = mod(u, 2), mod(u, SLOTS)
        return [
            remote(self.s2[j].at[s, at[k]], self.v3[j].at[v, k - 1], self.send.at[v, j, 11 + k], self.recv.at[v, j, 11 + k], dev[k])
            for k in (1, 2, 3)
        ]

    def start_core(self, u):
        self.core_copy(u).start()

    def spread(self, u):
        c = self.core_copy(u)
        c.wait_recv()
        s = mod(u, 2)
        roles = [[mod(n + 3 * UNITS - u - j, 3) for n in range(3)] for j in range(3)]
        at = [[[pick(roles[j][n], (8 * v, 2 * v, v // 2 * 32 + v % 2)) for v in range(4)] for n in range(2)] for j in range(3)]

        def body(z, _):
            last = (8 * z, 2 * z, div(z, 2) * 32 + mod(z, 2))
            for j, (lo, hi) in enumerate(LANES):
                base = pick(roles[j][2], last)
                for i in range(16):
                    n = base + (at[j][0][i % 4] + at[j][1][i // 4])
                    self.s0[j][s, n] = self.pbuf[z * 16 + i, self.p.core, :, lo:hi] + self.r0[s, z * 16 + i, :, lo:hi]
            return 0

        lax.fori_loop(0, 4, body, 0)
        for j in range(3):
            for copy in self.ring_copies(u, j, 0, range(4), self.line(u, j, 0)):
                copy.start()
        c.wait_send()

    def relay(self, u, level):
        src, dst = self.bufs(level)
        s, v = mod(u, 2), mod(u, SLOTS)
        for j in range(3):
            line = self.line(u, j, level)
            far = self.ring_copies(u, j, level, range(2), line)
            on = self.ring_copies(u, j, level, range(4, 6), line)
            for kind in range(2):
                blocks = self.piece(level, kind, line[0][(1, 3)[kind]])
                far[kind].wait_recv()
                src[j][s, blocks] = src[j][s, blocks] + dst[j][v, kind]
                on[kind].start()

    def settle(self, u, level):
        src, dst = self.bufs(level)
        s, v = mod(u, 2), mod(u, SLOTS)
        sent = []
        for j in range(3):
            line = self.line(u, j, level)
            copies = self.ring_copies(u, j, level, range(6), line)
            sent += copies
            for copy in copies[2:]:
                copy.wait_recv()
            for half in range(2):
                total = (src[j][s, self.piece(level, half, line[0][0])] + dst[j][v, 4 + half]) + dst[j][v, 3 - half]
                if level == 0:
                    self.s1[j][s, half * 8 : half * 8 + 8] = total
                else:
                    self.s2[j][s, half * 2 : half * 2 + 2] = total
            after = self.line(u, j, level + 1)
            for copy in self.last_copies(u, j, after) if level else self.ring_copies(u, j, 1, range(4), after):
                copy.start()
        for copy in sent:
            copy.wait_send()

    def finish(self, u, out_ref):
        s, v = mod(u, 2), mod(u, SLOTS)
        for j, (lo, hi) in enumerate(LANES):
            line = self.line(u, j, 2)
            copies = self.last_copies(u, j, line)
            for copy in copies:
                copy.wait_recv()
            total = (self.s2[j][s, line[0][0]] + self.v3[j][v, 0]) + (self.v3[j][v, 1] + self.v3[j][v, 2])
            out_ref[pl.ds(pl.multiple_of(u * ROWS, ROWS), ROWS), lo:hi] = total
            for copy in copies:
                copy.wait_send()


def main_kernel(h_ref, w_ref, tgt_ref, loss_ref, dh_ref, dw_ref, hb, wb, zb, dzb, acc, lse_col, tgt_col, lost,
                la, lb, h_sem, w_sem, out_sem, lsend, lrecv, *bufs):
    place = Place(lax.axis_index("fsdp") if COMM else jnp.minimum(tgt_ref[0, 0, 0], 0) + 5)
    stats = Stats(place, bufs[:4])
    rs = Scatter(place, bufs[4:])
    start = place.me * VOCAB
    blocks, quarter = SIZE // BLOCK, VOCAB // 4

    def load_h(t):
        return pltpu.make_async_copy(h_ref.at[:, t], hb.at[mod(t, 4)], h_sem.at[mod(t, 4)])

    load_w = pltpu.make_async_copy(w_ref, wb, w_sem)
    load_w.start()
    load_h(0).start()
    if COMM:
        barrier = place.greet()
    acc[...] = jnp.zeros_like(acc)
    lost[...] = jnp.zeros_like(lost)
    load_w.wait()

    lane = lax.broadcasted_iota(jnp.int32, (FEW, 128), 1)
    column = lax.broadcasted_iota(jnp.int32, (FEW, VOCAB), 1)

    def wide(x):
        return jnp.concatenate([x] * (VOCAB // 128), axis=1)

    def logits(t, rb):
        d = BLOCK // ROWS
        h = hb[mod(t, 4), rb * d : (rb + 1) * d].reshape(BLOCK, DIM)
        zb[mod(t, 3), rb * BLOCK : (rb + 1) * BLOCK, :] = dot(h, wb[...], 1, 1)

    def local_stats(t, n):
        z, s = mod(t, 3), mod(t, SLOTS)
        cols = []
        for r in range(n * 128, n * 128 + 128, FEW):
            x = zb[z, r : r + FEW, :]
            top = jnp.max(x, axis=1, keepdims=True)
            total = jnp.sum(jnp.exp(x - top), axis=1, keepdims=True)
            cols.append(jnp.where(lane == 0, top, total))
        packed = jnp.concatenate(cols, axis=0).T
        for i in range(2):
            stats.a[s, place.g, i, n : n + 1] = packed[i : i + 1]

    def columns(u):
        lse = stats.lse(u)
        for g in range(8):
            rows = slice(g * 128, (g + 1) * 128)
            lse_col[rows, :] = jnp.broadcast_to(lse[g : g + 1], (128, 128)).T
            tgt_col[rows, :] = jnp.broadcast_to(tgt_ref[u, g : g + 1, :] - start, (128, 128)).T

    def grad_logits(u, first, last):
        for r in range(first * 64, last * 64, FEW):
            rows = slice(r, r + FEW)
            x = zb[mod(u, 3), rows, :] - wide(lse_col[rows, :])
            hit = column == wide(tgt_col[rows, :])
            dzb[rows, :] = ((jnp.exp(x) - jnp.where(hit, 1.0, 0.0)) * (1.0 / TOKENS)).astype(BF16)
            found = jnp.where(hit, x, 0.0)
            lost[...] += sum(found[:, c : c + 128] for c in range(0, VOCAB, 128))

    def grad_hidden(rb):
        d = BLOCK // ROWS // 2
        rows = slice(rb * BLOCK, (rb + 1) * BLOCK)
        rs.pbuf[rb * d : (rb + 1) * d] = dot(dzb[rows, :], wb[...], 1, 0).reshape(d, 2, ROWS, DIM)

    def weight_block(u, n):
        cols = slice(n * quarter, (n + 1) * quarter)
        acc[:, cols] += dot(hb[mod(u, 4)].reshape(SIZE, DIM), dzb[:, cols], 0, 0)

    def when(cond, f, *args):
        if COMM:
            pl.when(cond)(lambda: f(*args))

    def step(t, _):
        u, old, older = t - 2, t - 3, t - 4
        early = t < UNITS
        ending = t >= UNITS

        @pl.when(t + 1 < UNITS)
        def _():
            load_h(t + 1).start()

        @pl.when(early)
        def _():
            load_h(t).wait()

        @pl.when(early)
        def logits_and_stats():
            for rb in range(blocks):
                logits(t, rb)
                if rb:
                    local_stats(t, 2 * rb - 2)
                    local_stats(t, 2 * rb - 1)
            local_stats(t, 2 * blocks - 2)
            local_stats(t, 2 * blocks - 1)

        if COMM:
            @pl.when(t == 0)
            def _():
                pl.semaphore_wait(barrier, 22)

        when(early, stats.start_first, t)
        when((t >= 1) & (t < 3), stats.start_second, t - 1)
        when(early & (old >= 0), rs.relay, old, 0)
        when(early & (older >= 0), rs.settle, older, 1)
        when(t >= 2, stats.wait_second, u)
        when(t == UNITS + 1, rs.relay, older, 1)

        @pl.when(t >= 2)
        def hidden():
            columns(u)
            grad_logits(u, 0, 4)
            for rb in range(blocks):
                grad_hidden(rb)
                if rb + 1 < blocks:
                    grad_logits(u, 4 * rb + 4, 4 * rb + 8)

        when(t >= 2, rs.start_core, u)
        when(ending, rs.relay, old, 0)
        when(ending, rs.settle, older, 1)
        when(early & (old >= 0), rs.settle, old, 0)
        when(early & (older >= 0), rs.finish, older, dh_ref)

        @pl.when((t >= 2) & (t < UNITS + 1))
        def weight():
            for n in range(4):
                weight_block(u, n)

        when(early & (old >= 0), rs.relay, old, 1)
        when(t == UNITS, rs.settle, old, 0)
        when(t == UNITS, rs.finish, older, dh_ref)
        when((t >= 2) & (t < UNITS + 1), rs.spread, u)
        when((t >= 2) & early, stats.start_second, t)
        return 0

    lax.fori_loop(0, UNITS + 2, step, 0)

    def to_rows(n):
        z, r = n // 2, n % 2 * quarter
        for i in range(0, quarter, 128):
            zb[z, r + i : r + i + 128, 0:DIM] = acc[:, n * quarter + i : n * quarter + i + 128].T
        put(n).start()

    def put(n):
        z, r = n // 2, n % 2 * quarter
        return pltpu.make_async_copy(
            zb.at[z, pl.ds(r, quarter), pl.ds(0, DIM)], dw_ref.at[pl.ds(n * quarter, quarter)], out_sem.at[n]
        )

    mine = jnp.sum(lost[...], axis=0, keepdims=True)
    if not COMM:
        for n in range(4):
            weight_block(7, n)
            to_rows(n)
        loss_ref[...] = jnp.sum(mine, axis=1, keepdims=True)
        for n in range(4):
            put(n).wait()
        return
    la[place.g] = mine
    row = [remote(la.at[place.g], la.at[place.g], lsend.at[k], lrecv.at[k], place.row[k]) for k in range(7)]
    plane = [remote(lb.at[place.q], lb.at[place.q], lsend.at[7 + k], lrecv.at[7 + k], place.plane[k]) for k in range(15)]
    for c in row:
        c.start()
    weight_block(7, 0)
    rs.settle(6, 0)
    rs.finish(5, dh_ref)
    weight_block(7, 1)
    rs.spread(7)
    weight_block(7, 2)
    to_rows(0)
    rs.relay(6, 1)
    rs.relay(7, 0)
    weight_block(7, 3)
    to_rows(1)
    for c in row:
        c.wait()
    lb[place.q] = functools.reduce(jnp.add, [la[k] for k in range(8)])
    for c in plane:
        c.start()
    rs.settle(7, 0)
    rs.settle(6, 1)
    to_rows(2)
    rs.relay(7, 1)
    rs.finish(6, dh_ref)
    to_rows(3)
    rs.settle(7, 1)
    for c in plane:
        c.wait()
    total = functools.reduce(jnp.add, [lb[k] for k in range(16)])
    loss_ref[...] = jnp.sum(total, axis=1, keepdims=True) * (-1.0 / TOKENS)
    rs.finish(7, dh_ref)
    for n in range(4):
        put(n).wait()


def fused(hidden, targets, w_blk):
    dma = pltpu.SemaphoreType.DMA
    any_spec, vmem = pl.BlockSpec(memory_space=pl.ANY), pl.BlockSpec(memory_space=pltpu.VMEM)
    return pl.pallas_call(
        main_kernel,
        out_shape=(
            jax.ShapeDtypeStruct((1, 1), F32),
            jax.ShapeDtypeStruct((64, DIM), F32),
            jax.ShapeDtypeStruct((VOCAB, DIM), F32),
        ),
        in_specs=[any_spec, any_spec, vmem],
        out_specs=(vmem, vmem, any_spec),
        scratch_shapes=[
            pltpu.VMEM((4, 128, ROWS, DIM), BF16),
            pltpu.VMEM((VOCAB, DIM), BF16),
            pltpu.VMEM((3, SIZE, VOCAB), F32),
            pltpu.VMEM((SIZE, VOCAB), BF16),
            pltpu.VMEM((DIM, VOCAB), F32),
            pltpu.VMEM((SIZE, 128), F32),
            pltpu.VMEM((SIZE, 128), jnp.int32),
            pltpu.VMEM((FEW, 128), F32),
            pltpu.VMEM((8, 1, 128), F32),
            pltpu.VMEM((16, 1, 128), F32),
            dma((4,)), dma, dma((4,)), dma((22,)), dma((22,)),
        ] + Stats.scratch() + Scatter.scratch(),
        compiler_params=pltpu.CompilerParams(
            vmem_limit_bytes=67043328, **(dict(collective_id=0, has_side_effects=True) if COMM else {})
        ),
    )(hidden, w_blk, targets)


def prepare(hidden, targets):
    h = hidden.reshape(128, UNITS, ROWS, DIM)
    t = targets.reshape(128, UNITS, ROWS).transpose(1, 0, 2).reshape(UNITS, 8, 128)
    return h, t


def solution(mesh):
    def local_step(hidden, targets, w_blk):
        h, t = prepare(hidden, targets)
        loss, grad_hid, grad_w = fused(h, t, w_blk)
        return loss.reshape(1), grad_hid, grad_w

    return jax.shard_map(
        local_step,
        mesh=mesh,
        in_specs=(P("data", None), P("data"), P("fsdp", None)),
        out_specs=(P("data"), P(("data", "fsdp"), None), P(("data", "fsdp"), None)),
        check_vma=False,
    )
```

```python
import functools

import jax
import jax.numpy as jnp
from jax import lax
from jax.experimental import pallas as pl
from jax.experimental.pallas import tpu as pltpu
from jax.sharding import PartitionSpec as P

MESH = pl.DeviceIdType.MESH
F32 = jnp.float32
BF16 = jnp.bfloat16
COMM = True

TOKENS, DIM, VOCAB = 8192, 640, 2048
UNITS, ROWS = 8, 8
SIZE = TOKENS // UNITS
BLOCK = 256
FEW = 16
PIECES = 8
SLOTS = 4
LANES = ((0, 256), (256, 512), (512, 640))
STRIDES = (2, 8, 32)


def mod(a, n):
    return a % n if isinstance(a, int) else lax.rem(a, jnp.int32(n))


def div(a, n):
    return a // n if isinstance(a, int) else lax.div(a, jnp.int32(n))


def dot(a, b, ca, cb):
    return lax.dot_general(a, b, (((ca,), (cb,)), ((), ())), preferred_element_type=F32)


def pick(n, values):
    return jnp.where(n == 0, values[0], jnp.where(n == 1, values[1], values[2]))


def remote(src, dst, send, recv, dev):
    return pltpu.make_async_remote_copy(
        src_ref=src, dst_ref=dst, send_sem=send, recv_sem=recv, device_id=(0, dev), device_id_type=MESH
    )


def merge(parts):
    top = functools.reduce(jnp.maximum, [p[0] for p in parts])
    total = functools.reduce(jnp.add, [p[1] * jnp.exp(p[0] - top) for p in parts])
    return top, total


class Place:
    def __init__(self, me):
        self.me = me
        self.g, self.q = mod(me, 8), div(me, 8)
        self.core = mod(me, 2)
        self.partner = me + 1 - 2 * self.core
        self.pos = (mod(div(me, 2), 4), mod(div(me, 8), 4), div(me, 32))
        self.row = [self.q * 8 + mod(self.g + k, 8) for k in range(1, 8)]
        self.plane = [mod(self.q + k, 16) * 8 + self.g for k in range(1, 16)]

    def along(self, axis):
        pos, stride = pick(axis, self.pos), pick(axis, STRIDES)
        at = [pos] + [mod(pos + k, 4) for k in (1, 2, 3)]
        return at, [self.me + (p - pos) * stride for p in at]

    def greet(self):
        barrier = pltpu.get_barrier_semaphore()
        for p in self.row + self.plane:
            pl.semaphore_signal(barrier, inc=1, device_id=(0, p), device_id_type=MESH)
        return barrier


class Stats:
    def __init__(self, place, bufs):
        self.p = place
        self.a, self.b, self.send, self.recv = bufs

    @staticmethod
    def scratch():
        dma = pltpu.SemaphoreType.DMA
        return [
            pltpu.VMEM((SLOTS, 8, 2, 8, 128), F32),
            pltpu.VMEM((SLOTS, 16, 2, 8, 128), F32),
            dma((SLOTS, 22)),
            dma((SLOTS, 22)),
        ]

    def first(self, t):
        s = mod(t, SLOTS)
        mine = self.a.at[s, self.p.g]
        return [remote(mine, mine, self.send.at[s, k], self.recv.at[s, k], self.p.row[k]) for k in range(7)]

    def second(self, t):
        s = mod(t, SLOTS)
        mine = self.b.at[s, self.p.q]
        return [remote(mine, mine, self.send.at[s, 7 + k], self.recv.at[s, 7 + k], self.p.plane[k]) for k in range(15)]

    def start_first(self, t):
        for c in self.first(t):
            c.start()

    def start_second(self, t):
        for c in self.first(t):
            c.wait()
        s = mod(t, SLOTS)
        self.b[s, self.p.q, 0], self.b[s, self.p.q, 1] = merge([self.a[s, k] for k in range(8)])
        for c in self.second(t):
            c.start()

    def wait_second(self, t):
        for c in self.second(t):
            c.wait()

    def lse(self, t):
        top, total = merge([self.b[mod(t, SLOTS), k] for k in range(16)])
        return top + jnp.log(total)


class Scatter:
    def __init__(self, place, bufs):
        self.p = place
        (self.pbuf, self.r0, self.s0, self.v1, self.s1, self.v2, self.s2, self.v3,
         self.csend, self.crecv, self.send, self.recv) = bufs

    @staticmethod
    def scratch():
        dma = pltpu.SemaphoreType.DMA
        widths = [b - a for a, b in LANES]
        return [
            pltpu.VMEM((64, 2, ROWS, DIM), F32),
            pltpu.VMEM((2, 64, ROWS, DIM), F32),
            [pltpu.VMEM((2, 64, ROWS, w), F32) for w in widths],
            [pltpu.VMEM((SLOTS, 6, 8, ROWS, w), F32) for w in widths],
            [pltpu.VMEM((2, 16, ROWS, w), F32) for w in widths],
            [pltpu.VMEM((SLOTS, 6, 2, ROWS, w), F32) for w in widths],
            [pltpu.VMEM((2, 4, ROWS, w), F32) for w in widths],
            [pltpu.VMEM((SLOTS, 3, ROWS, w), F32) for w in widths],
            dma((2,)), dma((2,)), dma((SLOTS, 3, 15)), dma((SLOTS, 3, 15)),
        ]

    def line(self, u, j, level):
        return self.p.along(mod(u + j + level, 3))

    def bufs(self, level):
        return ((self.s0, self.v1), (self.s1, self.v2))[level]

    def piece(self, level, half, owner):
        n = (8, 2)[level]
        return pl.ds((half * 4 + owner) * n, n)

    def core_copy(self, u):
        s = mod(u, 2)
        return remote(self.pbuf.at[:, 1 - self.p.core], self.r0.at[s], self.csend.at[s], self.crecv.at[s], self.p.partner)

    def ring_copies(self, u, j, level, kinds, line):
        src, dst = self.bufs(level)
        at, dev = line
        s, v = mod(u, 2), mod(u, SLOTS)
        copies = []
        for kind in kinds:
            half, step, way = ((0, 2, 1), (1, 2, 3), (1, 1, 1), (0, 3, 3), (0, 1, 1), (1, 3, 3))[kind]
            n = level * 6 + kind
            copies.append(remote(
                src[j].at[s, self.piece(level, half, at[step])], dst[j].at[v, kind], self.send.at[v, j, n],
                self.recv.at[v, j, n], dev[way],
            ))
        return copies

    def last_copies(self, u, j, line):
        at, dev = line
        s, v = mod(u, 2), mod(u, SLOTS)
        return [
            remote(self.s2[j].at[s, at[k]], self.v3[j].at[v, k - 1], self.send.at[v, j, 11 + k], self.recv.at[v, j, 11 + k], dev[k])
            for k in (1, 2, 3)
        ]

    def start_core(self, u):
        self.core_copy(u).start()

    def spread(self, u):
        c = self.core_copy(u)
        c.wait_recv()
        s = mod(u, 2)
        roles = [[mod(n + 3 * UNITS - u - j, 3) for n in range(3)] for j in range(3)]
        at = [[[pick(roles[j][n], (8 * v, 2 * v, v // 2 * 32 + v % 2)) for v in range(4)] for n in range(2)] for j in range(3)]

        def body(z, _):
            last = (8 * z, 2 * z, div(z, 2) * 32 + mod(z, 2))
            for j, (lo, hi) in enumerate(LANES):
                base = pick(roles[j][2], last)
                for i in range(16):
                    n = base + (at[j][0][i % 4] + at[j][1][i // 4])
                    self.s0[j][s, n] = self.pbuf[z * 16 + i, self.p.core, :, lo:hi] + self.r0[s, z * 16 + i, :, lo:hi]
            return 0

        lax.fori_loop(0, 4, body, 0)
        for j in range(3):
            for copy in self.ring_copies(u, j, 0, range(4), self.line(u, j, 0)):
                copy.start()
        c.wait_send()

    def relay(self, u, level):
        src, dst = self.bufs(level)
        s, v = mod(u, 2), mod(u, SLOTS)
        for j in range(3):
            line = self.line(u, j, level)
            far = self.ring_copies(u, j, level, range(2), line)
            on = self.ring_copies(u, j, level, range(4, 6), line)
            for kind in range(2):
                blocks = self.piece(level, kind, line[0][(1, 3)[kind]])
                far[kind].wait_recv()
                src[j][s, blocks] = src[j][s, blocks] + dst[j][v, kind]
                on[kind].start()

    def settle(self, u, level):
        src, dst = self.bufs(level)
        s, v = mod(u, 2), mod(u, SLOTS)
        sent = []
        for j in range(3):
            line = self.line(u, j, level)
            copies = self.ring_copies(u, j, level, range(6), line)
            sent += copies
            for copy in copies[2:]:
                copy.wait_recv()
            for half in range(2):
                total = (src[j][s, self.piece(level, half, line[0][0])] + dst[j][v, 4 + half]) + dst[j][v, 3 - half]
                if level == 0:
                    self.s1[j][s, half * 8 : half * 8 + 8] = total
                else:
                    self.s2[j][s, half * 2 : half * 2 + 2] = total
            after = self.line(u, j, level + 1)
            for copy in self.last_copies(u, j, after) if level else self.ring_copies(u, j, 1, range(4), after):
                copy.start()
        for copy in sent:
            copy.wait_send()

    def finish(self, u, out_ref):
        s, v = mod(u, 2), mod(u, SLOTS)
        for j, (lo, hi) in enumerate(LANES):
            line = self.line(u, j, 2)
            copies = self.last_copies(u, j, line)
            for copy in copies:
                copy.wait_recv()
            total = (self.s2[j][s, line[0][0]] + self.v3[j][v, 0]) + (self.v3[j][v, 1] + self.v3[j][v, 2])
            out_ref[pl.ds(pl.multiple_of(u * ROWS, ROWS), ROWS), lo:hi] = total
            for copy in copies:
                copy.wait_send()


def main_kernel(h_ref, w_ref, tgt_ref, loss_ref, dh_ref, dw_ref, hb, wb, zb, dzb, acc, lse_col, tgt_col, lost,
                la, lb, h_sem, w_sem, out_sem, lsend, lrecv, *bufs):
    place = Place(lax.axis_index("fsdp") if COMM else jnp.minimum(tgt_ref[0, 0, 0], 0) + 5)
    stats = Stats(place, bufs[:4])
    rs = Scatter(place, bufs[4:])
    start = place.me * VOCAB
    blocks, quarter = SIZE // BLOCK, VOCAB // 4

    def load_h(t):
        return pltpu.make_async_copy(h_ref.at[:, t], hb.at[mod(t, 4)], h_sem.at[mod(t, 4)])

    load_w = pltpu.make_async_copy(w_ref, wb, w_sem)
    load_w.start()
    load_h(0).start()
    if COMM:
        barrier = place.greet()
    acc[...] = jnp.zeros_like(acc)
    lost[...] = jnp.zeros_like(lost)
    load_w.wait()

    lane = lax.broadcasted_iota(jnp.int32, (FEW, 128), 1)
    column = lax.broadcasted_iota(jnp.int32, (FEW, VOCAB), 1)

    def wide(x):
        return jnp.concatenate([x] * (VOCAB // 128), axis=1)

    def logits(t, rb):
        d = BLOCK // ROWS
        h = hb[mod(t, 4), rb * d : (rb + 1) * d].reshape(BLOCK, DIM)
        zb[mod(t, 3), rb * BLOCK : (rb + 1) * BLOCK, :] = dot(h, wb[...], 1, 1)

    def local_stats(t, n):
        z, s = mod(t, 3), mod(t, SLOTS)
        cols = []
        for r in range(n * 128, n * 128 + 128, FEW):
            x = zb[z, r : r + FEW, :]
            top = jnp.max(x, axis=1, keepdims=True)
            total = jnp.sum(jnp.exp(x - top), axis=1, keepdims=True)
            cols.append(jnp.where(lane == 0, top, total))
        packed = jnp.concatenate(cols, axis=0).T
        for i in range(2):
            stats.a[s, place.g, i, n : n + 1] = packed[i : i + 1]

    def columns(u):
        lse = stats.lse(u)
        for g in range(8):
            rows = slice(g * 128, (g + 1) * 128)
            lse_col[rows, :] = jnp.broadcast_to(lse[g : g + 1], (128, 128)).T
            tgt_col[rows, :] = jnp.broadcast_to(tgt_ref[u, g : g + 1, :] - start, (128, 128)).T

    def grad_logits(u, first, last):
        for r in range(first * 64, last * 64, FEW):
            rows = slice(r, r + FEW)
            x = zb[mod(u, 3), rows, :] - wide(lse_col[rows, :])
            hit = column == wide(tgt_col[rows, :])
            dzb[mod(u, 2), rows, :] = ((jnp.exp(x) - jnp.where(hit, 1.0, 0.0)) * (1.0 / TOKENS)).astype(BF16)
            found = jnp.where(hit, x, 0.0)
            lost[...] += sum(found[:, c : c + 128] for c in range(0, VOCAB, 128))

    def grad_hidden(u, rb):
        d = BLOCK // ROWS // 2
        rows = slice(rb * BLOCK, (rb + 1) * BLOCK)
        rs.pbuf[rb * d : (rb + 1) * d] = dot(dzb[mod(u, 2), rows, :], wb[...], 1, 0).reshape(d, 2, ROWS, DIM)

    def weight_block(u, n):
        cols = slice(n * quarter, (n + 1) * quarter)
        acc[:, cols] += dot(hb[mod(u, 4)].reshape(SIZE, DIM), dzb[mod(u, 2), :, cols], 0, 0)

    def when(cond, f, *args):
        if COMM:
            pl.when(cond)(lambda: f(*args))

    def step(t, _):
        u, old, older = t - 2, t - 3, t - 4
        early = t < UNITS
        ending = t >= UNITS

        @pl.when(early)
        def _():
            load_h(t).wait()

        @pl.when(early)
        def logits_and_stats():
            for rb in range(blocks):
                logits(t, rb)
                if rb:
                    local_stats(t, 2 * rb - 2)
                    local_stats(t, 2 * rb - 1)
            local_stats(t, 2 * blocks - 2)
            local_stats(t, 2 * blocks - 1)

        if COMM:
            @pl.when(t == 0)
            def _():
                pl.semaphore_wait(barrier, 22)

        when(old >= 0, rs.spread, old)
        when(early, stats.start_first, t)
        when((t >= 1) & (t < 3), stats.start_second, t - 1)
        when(early & (older >= 0), rs.relay, older, 1)
        when(t == UNITS + 1, rs.finish, UNITS - 4, dh_ref)
        when(t >= 2, stats.wait_second, u)

        @pl.when(t >= 2)
        def hidden():
            columns(u)
            grad_logits(u, 0, 4)
            for rb in range(blocks):
                grad_hidden(u, rb)
                if rb + 1 < blocks:
                    grad_logits(u, 4 * rb + 4, 4 * rb + 8)

        when(t >= 2, rs.start_core, u)
        when(old >= 0, rs.relay, old, 0)
        when(ending, rs.relay, older, 1)
        when(early & (older >= 0), rs.settle, older, 1)

        @pl.when(old >= 0)
        def weight():
            for n in range(4):
                weight_block(old, n)

        @pl.when(t + 1 < UNITS)
        def _():
            load_h(t + 1).start()

        when(old >= 0, rs.settle, old, 0)
        when(ending, rs.settle, older, 1)
        when((t < UNITS) & (older >= 0), rs.finish, older, dh_ref)
        when((t >= 2) & early, stats.start_second, t)
        return 0

    lax.fori_loop(0, UNITS + 2, step, 0)

    def to_rows(n):
        z, r = n // 2, n % 2 * quarter
        for i in range(0, quarter, 128):
            zb[z, r + i : r + i + 128, 0:DIM] = acc[:, n * quarter + i : n * quarter + i + 128].T
        put(n).start()

    def put(n):
        z, r = n // 2, n % 2 * quarter
        return pltpu.make_async_copy(
            zb.at[z, pl.ds(r, quarter), pl.ds(0, DIM)], dw_ref.at[pl.ds(n * quarter, quarter)], out_sem.at[n]
        )

    mine = jnp.sum(lost[...], axis=0, keepdims=True)
    if not COMM:
        for n in range(4):
            weight_block(7, n)
            to_rows(n)
        loss_ref[...] = jnp.sum(mine, axis=1, keepdims=True)
        for n in range(4):
            put(n).wait()
        return
    la[place.g] = mine
    row = [remote(la.at[place.g], la.at[place.g], lsend.at[k], lrecv.at[k], place.row[k]) for k in range(7)]
    plane = [remote(lb.at[place.q], lb.at[place.q], lsend.at[7 + k], lrecv.at[7 + k], place.plane[k]) for k in range(15)]
    for c in row:
        c.start()
    weight_block(7, 0)
    rs.spread(7)
    rs.finish(5, dh_ref)
    weight_block(7, 1)
    rs.relay(7, 0)
    rs.relay(6, 1)
    weight_block(7, 2)
    to_rows(0)
    for c in row:
        c.wait()
    lb[place.q] = functools.reduce(jnp.add, [la[k] for k in range(8)])
    for c in plane:
        c.start()
    rs.settle(7, 0)
    rs.settle(6, 1)
    weight_block(7, 3)
    to_rows(1)
    rs.relay(7, 1)
    rs.finish(6, dh_ref)
    to_rows(2)
    to_rows(3)
    rs.settle(7, 1)
    for c in plane:
        c.wait()
    total = functools.reduce(jnp.add, [lb[k] for k in range(16)])
    loss_ref[...] = jnp.sum(total, axis=1, keepdims=True) * (-1.0 / TOKENS)
    rs.finish(7, dh_ref)
    for n in range(4):
        put(n).wait()


def fused(hidden, targets, w_blk):
    dma = pltpu.SemaphoreType.DMA
    any_spec, vmem = pl.BlockSpec(memory_space=pl.ANY), pl.BlockSpec(memory_space=pltpu.VMEM)
    return pl.pallas_call(
        main_kernel,
        out_shape=(
            jax.ShapeDtypeStruct((1, 1), F32),
            jax.ShapeDtypeStruct((64, DIM), F32),
            jax.ShapeDtypeStruct((VOCAB, DIM), F32),
        ),
        in_specs=[any_spec, any_spec, vmem],
        out_specs=(vmem, vmem, any_spec),
        scratch_shapes=[
            pltpu.VMEM((4, 128, ROWS, DIM), BF16),
            pltpu.VMEM((VOCAB, DIM), BF16),
            pltpu.VMEM((3, SIZE, VOCAB), F32),
            pltpu.VMEM((2, SIZE, VOCAB), BF16),
            pltpu.VMEM((DIM, VOCAB), F32),
            pltpu.VMEM((SIZE, 128), F32),
            pltpu.VMEM((SIZE, 128), jnp.int32),
            pltpu.VMEM((FEW, 128), F32),
            pltpu.VMEM((8, 1, 128), F32),
            pltpu.VMEM((16, 1, 128), F32),
            dma((4,)), dma, dma((4,)), dma((22,)), dma((22,)),
        ] + Stats.scratch() + Scatter.scratch(),
        compiler_params=pltpu.CompilerParams(
            vmem_limit_bytes=67043328, **(dict(collective_id=0, has_side_effects=True) if COMM else {})
        ),
    )(hidden, w_blk, targets)


def deliver_kernel(loss_in, dh_in, dw_in, loss_out, dh_out, dw_out, buf, load, store):
    rows = VOCAB // PIECES
    at = [pl.ds(n * rows, rows) for n in range(PIECES)]
    loads = [pltpu.make_async_copy(dw_in.at[a], buf.at[a], load.at[n]) for n, a in enumerate(at)]
    stores = [pltpu.make_async_copy(buf.at[a], dw_out.at[a], store.at[n]) for n, a in enumerate(at)]
    for copy in loads:
        copy.start()
    loss_out[...] = loss_in[...]
    dh_out[...] = dh_in[...]
    for one, other in zip(loads, stores):
        one.wait()
        other.start()
    for copy in stores:
        copy.wait()


def deliver(loss, grad_hid, grad_w):
    any_spec, vmem = pl.BlockSpec(memory_space=pl.ANY), pl.BlockSpec(memory_space=pltpu.VMEM)
    dma = pltpu.SemaphoreType.DMA
    return pl.pallas_call(
        deliver_kernel,
        out_shape=tuple(jax.ShapeDtypeStruct(x.shape, F32) for x in (loss, grad_hid, grad_w)),
        in_specs=[vmem, vmem, any_spec],
        out_specs=(vmem, vmem, any_spec),
        scratch_shapes=[pltpu.VMEM((VOCAB, DIM), F32), dma((PIECES,)), dma((PIECES,))],
    )(loss, grad_hid, grad_w)


def prepare(hidden, targets):
    h = hidden.reshape(128, UNITS, ROWS, DIM)
    t = targets.reshape(128, UNITS, ROWS).transpose(1, 0, 2).reshape(UNITS, 8, 128)
    return h, t


def solution(mesh):
    def local_step(hidden, targets, w_blk):
        h, t = prepare(hidden, targets)
        loss, grad_hid, grad_w = deliver(*fused(h, t, w_blk))
        return loss.reshape(1), grad_hid, grad_w

    return jax.shard_map(
        local_step,
        mesh=mesh,
        in_specs=(P("data", None), P("data"), P("fsdp", None)),
        out_specs=(P("data"), P(("data", "fsdp"), None), P(("data", "fsdp"), None)),
        check_vma=False,
    )
```

```python
import functools

import jax
import jax.numpy as jnp
from jax import lax
from jax.experimental import pallas as pl
from jax.experimental.pallas import tpu as pltpu
from jax.sharding import PartitionSpec as P

MESH = pl.DeviceIdType.MESH
F32 = jnp.float32
BF16 = jnp.bfloat16
COMM = True

TOKENS, DIM, VOCAB = 8192, 640, 2048
UNITS, ROWS = 8, 8
SIZE = TOKENS // UNITS
BLOCK = 256
FEW = 16
PIECES = 8
SLOTS = 4
LANES = ((0, 256), (256, 512), (512, 640))
STRIDES = (2, 8, 32)


def mod(a, n):
    return a % n if isinstance(a, int) else lax.rem(a, jnp.int32(n))


def div(a, n):
    return a // n if isinstance(a, int) else lax.div(a, jnp.int32(n))


def dot(a, b, ca, cb):
    return lax.dot_general(a, b, (((ca,), (cb,)), ((), ())), preferred_element_type=F32)


def pick(n, values):
    return jnp.where(n == 0, values[0], jnp.where(n == 1, values[1], values[2]))


def remote(src, dst, send, recv, dev):
    return pltpu.make_async_remote_copy(
        src_ref=src, dst_ref=dst, send_sem=send, recv_sem=recv, device_id=(0, dev), device_id_type=MESH
    )


def merge(parts):
    top = functools.reduce(jnp.maximum, [p[0] for p in parts])
    total = functools.reduce(jnp.add, [p[1] * jnp.exp(p[0] - top) for p in parts])
    return top, total


class Place:
    def __init__(self, me):
        self.me = me
        self.g, self.q = mod(me, 8), div(me, 8)
        self.core = mod(me, 2)
        self.partner = me + 1 - 2 * self.core
        self.pos = (mod(div(me, 2), 4), mod(div(me, 8), 4), div(me, 32))
        self.row = [self.q * 8 + mod(self.g + k, 8) for k in range(1, 8)]
        self.plane = [mod(self.q + k, 16) * 8 + self.g for k in range(1, 16)]

    def along(self, axis):
        pos, stride = pick(axis, self.pos), pick(axis, STRIDES)
        at = [pos] + [mod(pos + k, 4) for k in (1, 2, 3)]
        return at, [self.me + (p - pos) * stride for p in at]

    def greet(self):
        barrier = pltpu.get_barrier_semaphore()
        for p in self.row + self.plane:
            pl.semaphore_signal(barrier, inc=1, device_id=(0, p), device_id_type=MESH)
        return barrier


class Stats:
    def __init__(self, place, bufs):
        self.p = place
        self.a, self.b, self.send, self.recv = bufs

    @staticmethod
    def scratch():
        dma = pltpu.SemaphoreType.DMA
        return [
            pltpu.VMEM((SLOTS, 8, 2, 8, 128), F32),
            pltpu.VMEM((SLOTS, 16, 2, 8, 128), F32),
            dma((SLOTS, 22)),
            dma((SLOTS, 22)),
        ]

    def first(self, t):
        s = mod(t, SLOTS)
        mine = self.a.at[s, self.p.g]
        return [remote(mine, mine, self.send.at[s, k], self.recv.at[s, k], self.p.row[k]) for k in range(7)]

    def second(self, t):
        s = mod(t, SLOTS)
        mine = self.b.at[s, self.p.q]
        return [remote(mine, mine, self.send.at[s, 7 + k], self.recv.at[s, 7 + k], self.p.plane[k]) for k in range(15)]

    def start_first(self, t):
        for c in self.first(t):
            c.start()

    def start_second(self, t):
        for c in self.first(t):
            c.wait()
        s = mod(t, SLOTS)
        self.b[s, self.p.q, 0], self.b[s, self.p.q, 1] = merge([self.a[s, k] for k in range(8)])
        for c in self.second(t):
            c.start()

    def wait_second(self, t):
        for c in self.second(t):
            c.wait()

    def lse(self, t):
        top, total = merge([self.b[mod(t, SLOTS), k] for k in range(16)])
        return top + jnp.log(total)


class Scatter:
    def __init__(self, place, bufs):
        self.p = place
        (self.pbuf, self.r0, self.s0, self.v1, self.s1, self.v2, self.s2, self.v3,
         self.csend, self.crecv, self.send, self.recv) = bufs

    @staticmethod
    def scratch():
        dma = pltpu.SemaphoreType.DMA
        widths = [b - a for a, b in LANES]
        return [
            pltpu.VMEM((64, 2, ROWS, DIM), F32),
            pltpu.VMEM((2, 64, ROWS, DIM), F32),
            [pltpu.VMEM((2, 64, ROWS, w), F32) for w in widths],
            [pltpu.VMEM((SLOTS, 6, 8, ROWS, w), F32) for w in widths],
            [pltpu.VMEM((2, 16, ROWS, w), F32) for w in widths],
            [pltpu.VMEM((SLOTS, 6, 2, ROWS, w), F32) for w in widths],
            [pltpu.VMEM((2, 4, ROWS, w), F32) for w in widths],
            [pltpu.VMEM((SLOTS, 3, ROWS, w), F32) for w in widths],
            dma((2,)), dma((2,)), dma((SLOTS, 3, 15)), dma((SLOTS, 3, 15)),
        ]

    def line(self, u, j, level):
        return self.p.along(mod(u + j + level, 3))

    def bufs(self, level):
        return ((self.s0, self.v1), (self.s1, self.v2))[level]

    def piece(self, level, half, owner):
        n = (8, 2)[level]
        return pl.ds((half * 4 + owner) * n, n)

    def core_copy(self, u):
        s = mod(u, 2)
        return remote(self.pbuf.at[:, 1 - self.p.core], self.r0.at[s], self.csend.at[s], self.crecv.at[s], self.p.partner)

    def ring_copies(self, u, j, level, kinds, line):
        src, dst = self.bufs(level)
        at, dev = line
        s, v = mod(u, 2), mod(u, SLOTS)
        copies = []
        for kind in kinds:
            half, step, way = ((0, 2, 1), (1, 2, 3), (1, 1, 1), (0, 3, 3), (0, 1, 1), (1, 3, 3))[kind]
            n = level * 6 + kind
            copies.append(remote(
                src[j].at[s, self.piece(level, half, at[step])], dst[j].at[v, kind], self.send.at[v, j, n],
                self.recv.at[v, j, n], dev[way],
            ))
        return copies

    def last_copies(self, u, j, line):
        at, dev = line
        s, v = mod(u, 2), mod(u, SLOTS)
        return [
            remote(self.s2[j].at[s, at[k]], self.v3[j].at[v, k - 1], self.send.at[v, j, 11 + k], self.recv.at[v, j, 11 + k], dev[k])
            for k in (1, 2, 3)
        ]

    def start_core(self, u):
        self.core_copy(u).start()

    def spread(self, u):
        c = self.core_copy(u)
        c.wait_recv()
        s = mod(u, 2)
        roles = [[mod(n + 3 * UNITS - u - j, 3) for n in range(3)] for j in range(3)]
        at = [[[pick(roles[j][n], (8 * v, 2 * v, v // 2 * 32 + v % 2)) for v in range(4)] for n in range(2)] for j in range(3)]

        def body(z, _):
            last = (8 * z, 2 * z, div(z, 2) * 32 + mod(z, 2))
            for j, (lo, hi) in enumerate(LANES):
                base = pick(roles[j][2], last)
                for i in range(16):
                    n = base + (at[j][0][i % 4] + at[j][1][i // 4])
                    self.s0[j][s, n] = self.pbuf[z * 16 + i, self.p.core, :, lo:hi] + self.r0[s, z * 16 + i, :, lo:hi]
            return 0

        lax.fori_loop(0, 4, body, 0)
        for j in range(3):
            for copy in self.ring_copies(u, j, 0, range(4), self.line(u, j, 0)):
                copy.start()
        c.wait_send()

    def relay(self, u, level):
        src, dst = self.bufs(level)
        s, v = mod(u, 2), mod(u, SLOTS)
        for j in range(3):
            line = self.line(u, j, level)
            far = self.ring_copies(u, j, level, range(2), line)
            on = self.ring_copies(u, j, level, range(4, 6), line)
            for kind in range(2):
                blocks = self.piece(level, kind, line[0][(1, 3)[kind]])
                far[kind].wait_recv()
                src[j][s, blocks] = src[j][s, blocks] + dst[j][v, kind]
                on[kind].start()

    def settle(self, u, level):
        src, dst = self.bufs(level)
        s, v = mod(u, 2), mod(u, SLOTS)
        sent = []
        for j in range(3):
            line = self.line(u, j, level)
            copies = self.ring_copies(u, j, level, range(6), line)
            sent += copies
            for copy in copies[2:]:
                copy.wait_recv()
            for half in range(2):
                total = (src[j][s, self.piece(level, half, line[0][0])] + dst[j][v, 4 + half]) + dst[j][v, 3 - half]
                if level == 0:
                    self.s1[j][s, half * 8 : half * 8 + 8] = total
                else:
                    self.s2[j][s, half * 2 : half * 2 + 2] = total
            after = self.line(u, j, level + 1)
            for copy in self.last_copies(u, j, after) if level else self.ring_copies(u, j, 1, range(4), after):
                copy.start()
        for copy in sent:
            copy.wait_send()

    def finish(self, u, out_ref):
        s, v = mod(u, 2), mod(u, SLOTS)
        for j, (lo, hi) in enumerate(LANES):
            line = self.line(u, j, 2)
            copies = self.last_copies(u, j, line)
            for copy in copies:
                copy.wait_recv()
            total = (self.s2[j][s, line[0][0]] + self.v3[j][v, 0]) + (self.v3[j][v, 1] + self.v3[j][v, 2])
            out_ref[pl.ds(pl.multiple_of(u * ROWS, ROWS), ROWS), lo:hi] = total
            for copy in copies:
                copy.wait_send()


def main_kernel(h_ref, w_ref, tgt_ref, loss_ref, dh_ref, dw_ref, hb, wb, zb, dzb, acc, lse_col, tgt_col, lost,
                la, lb, h_sem, w_sem, out_sem, lsend, lrecv, *bufs):
    place = Place(lax.axis_index("fsdp") if COMM else jnp.minimum(tgt_ref[0, 0, 0], 0) + 5)
    stats = Stats(place, bufs[:4])
    rs = Scatter(place, bufs[4:])
    start = place.me * VOCAB
    blocks, quarter = SIZE // BLOCK, VOCAB // 4

    def load_h(t):
        return pltpu.make_async_copy(h_ref.at[:, t], hb.at[mod(t, 4)], h_sem.at[mod(t, 4)])

    load_w = pltpu.make_async_copy(w_ref, wb, w_sem)
    load_w.start()
    load_h(0).start()
    if COMM:
        barrier = place.greet()
    acc[...] = jnp.zeros_like(acc)
    lost[...] = jnp.zeros_like(lost)
    load_w.wait()

    lane = lax.broadcasted_iota(jnp.int32, (FEW, 128), 1)
    column = lax.broadcasted_iota(jnp.int32, (FEW, VOCAB), 1)

    def wide(x):
        return jnp.concatenate([x] * (VOCAB // 128), axis=1)

    def logits(t, rb):
        d = BLOCK // ROWS
        h = hb[mod(t, 4), rb * d : (rb + 1) * d].reshape(BLOCK, DIM)
        zb[mod(t, 3), rb * BLOCK : (rb + 1) * BLOCK, :] = dot(h, wb[...], 1, 1)

    def local_stats(t, n):
        z, s = mod(t, 3), mod(t, SLOTS)
        cols = []
        for r in range(n * 128, n * 128 + 128, FEW):
            x = zb[z, r : r + FEW, :]
            top = jnp.max(x, axis=1, keepdims=True)
            total = jnp.sum(jnp.exp(x - top), axis=1, keepdims=True)
            cols.append(jnp.where(lane == 0, top, total))
        packed = jnp.concatenate(cols, axis=0).T
        for i in range(2):
            stats.a[s, place.g, i, n : n + 1] = packed[i : i + 1]

    def columns(u):
        lse = stats.lse(u)
        for g in range(8):
            rows = slice(g * 128, (g + 1) * 128)
            lse_col[rows, :] = jnp.broadcast_to(lse[g : g + 1], (128, 128)).T
            tgt_col[rows, :] = jnp.broadcast_to(tgt_ref[u, g : g + 1, :] - start, (128, 128)).T

    def grad_logits(u, first, last):
        for r in range(first * 64, last * 64, FEW):
            rows = slice(r, r + FEW)
            x = zb[mod(u, 3), rows, :] - wide(lse_col[rows, :])
            hit = column == wide(tgt_col[rows, :])
            dzb[rows, :] = ((jnp.exp(x) - jnp.where(hit, 1.0, 0.0)) * (1.0 / TOKENS)).astype(BF16)
            found = jnp.where(hit, x, 0.0)
            lost[...] += sum(found[:, c : c + 128] for c in range(0, VOCAB, 128))

    def grad_hidden(rb):
        d = BLOCK // ROWS // 2
        rows = slice(rb * BLOCK, (rb + 1) * BLOCK)
        rs.pbuf[rb * d : (rb + 1) * d] = dot(dzb[rows, :], wb[...], 1, 0).reshape(d, 2, ROWS, DIM)

    def weight_block(u, n):
        cols = slice(n * quarter, (n + 1) * quarter)
        acc[:, cols] += dot(hb[mod(u, 4)].reshape(SIZE, DIM), dzb[:, cols], 0, 0)

    def when(cond, f, *args):
        if COMM:
            pl.when(cond)(lambda: f(*args))

    def step(t, _):
        u, old, older = t - 2, t - 3, t - 4
        early = t < UNITS
        ending = t >= UNITS

        @pl.when(t + 1 < UNITS)
        def _():
            load_h(t + 1).start()

        @pl.when(early)
        def _():
            load_h(t).wait()

        @pl.when(early)
        def logits_and_stats():
            for rb in range(blocks):
                logits(t, rb)
                if rb:
                    local_stats(t, 2 * rb - 2)
                    local_stats(t, 2 * rb - 1)
            local_stats(t, 2 * blocks - 2)
            local_stats(t, 2 * blocks - 1)

        if COMM:
            @pl.when(t == 0)
            def _():
                pl.semaphore_wait(barrier, 22)

        when(early, stats.start_first, t)
        when((t >= 1) & (t < 3), stats.start_second, t - 1)
        when(early & (old >= 0), rs.relay, old, 0)
        when(early & (older >= 0), rs.settle, older, 1)
        when(t >= 2, stats.wait_second, u)
        when(t == UNITS + 1, rs.relay, older, 1)

        @pl.when(t >= 2)
        def hidden():
            columns(u)
            grad_logits(u, 0, 4)
            for rb in range(blocks):
                grad_hidden(rb)
                if rb + 1 < blocks:
                    grad_logits(u, 4 * rb + 4, 4 * rb + 8)

        when(t >= 2, rs.start_core, u)
        when(ending, rs.relay, old, 0)
        when(ending, rs.settle, older, 1)
        when(early & (old >= 0), rs.settle, old, 0)
        when(early & (older >= 0), rs.finish, older, dh_ref)

        @pl.when((t >= 2) & (t < UNITS + 1))
        def weight():
            for n in range(4):
                weight_block(u, n)

        when(early & (old >= 0), rs.relay, old, 1)
        when(t == UNITS, rs.settle, old, 0)
        when(t == UNITS, rs.finish, older, dh_ref)
        when((t >= 2) & (t < UNITS + 1), rs.spread, u)
        when((t >= 2) & early, stats.start_second, t)
        return 0

    lax.fori_loop(0, UNITS + 2, step, 0)

    def to_rows(n):
        z, r = n // 2, n % 2 * quarter
        for i in range(0, quarter, 128):
            zb[z, r + i : r + i + 128, 0:DIM] = acc[:, n * quarter + i : n * quarter + i + 128].T
        put(n).start()

    def put(n):
        z, r = n // 2, n % 2 * quarter
        return pltpu.make_async_copy(
            zb.at[z, pl.ds(r, quarter), pl.ds(0, DIM)], dw_ref.at[pl.ds(n * quarter, quarter)], out_sem.at[n]
        )

    mine = jnp.sum(lost[...], axis=0, keepdims=True)
    if not COMM:
        for n in range(4):
            weight_block(7, n)
            to_rows(n)
        loss_ref[...] = jnp.sum(mine, axis=1, keepdims=True)
        for n in range(4):
            put(n).wait()
        return
    la[place.g] = mine
    row = [remote(la.at[place.g], la.at[place.g], lsend.at[k], lrecv.at[k], place.row[k]) for k in range(7)]
    plane = [remote(lb.at[place.q], lb.at[place.q], lsend.at[7 + k], lrecv.at[7 + k], place.plane[k]) for k in range(15)]
    for c in row:
        c.start()
    weight_block(7, 0)
    rs.settle(6, 0)
    rs.finish(5, dh_ref)
    weight_block(7, 1)
    rs.spread(7)
    weight_block(7, 2)
    to_rows(0)
    rs.relay(6, 1)
    rs.relay(7, 0)
    weight_block(7, 3)
    to_rows(1)
    for c in row:
        c.wait()
    lb[place.q] = functools.reduce(jnp.add, [la[k] for k in range(8)])
    for c in plane:
        c.start()
    rs.settle(7, 0)
    rs.settle(6, 1)
    to_rows(2)
    rs.relay(7, 1)
    rs.finish(6, dh_ref)
    to_rows(3)
    rs.settle(7, 1)
    for c in plane:
        c.wait()
    total = functools.reduce(jnp.add, [lb[k] for k in range(16)])
    loss_ref[...] = jnp.sum(total, axis=1, keepdims=True) * (-1.0 / TOKENS)
    rs.finish(7, dh_ref)
    for n in range(4):
        put(n).wait()


def fused(hidden, targets, w_blk):
    dma = pltpu.SemaphoreType.DMA
    any_spec, vmem = pl.BlockSpec(memory_space=pl.ANY), pl.BlockSpec(memory_space=pltpu.VMEM)
    return pl.pallas_call(
        main_kernel,
        out_shape=(
            jax.ShapeDtypeStruct((1, 1), F32),
            jax.ShapeDtypeStruct((64, DIM), F32),
            jax.ShapeDtypeStruct((VOCAB, DIM), F32),
        ),
        in_specs=[any_spec, any_spec, vmem],
        out_specs=(vmem, vmem, any_spec),
        scratch_shapes=[
            pltpu.VMEM((4, 128, ROWS, DIM), BF16),
            pltpu.VMEM((VOCAB, DIM), BF16),
            pltpu.VMEM((3, SIZE, VOCAB), F32),
            pltpu.VMEM((SIZE, VOCAB), BF16),
            pltpu.VMEM((DIM, VOCAB), F32),
            pltpu.VMEM((SIZE, 128), F32),
            pltpu.VMEM((SIZE, 128), jnp.int32),
            pltpu.VMEM((FEW, 128), F32),
            pltpu.VMEM((8, 1, 128), F32),
            pltpu.VMEM((16, 1, 128), F32),
            dma((4,)), dma, dma((4,)), dma((22,)), dma((22,)),
        ] + Stats.scratch() + Scatter.scratch(),
        compiler_params=pltpu.CompilerParams(
            vmem_limit_bytes=67043328, **(dict(collective_id=0, has_side_effects=True) if COMM else {})
        ),
    )(hidden, w_blk, targets)


def deliver_kernel(dh_in, dw_in, dh_out, dw_out, dh_buf, dw_buf, load, store):
    rows = VOCAB // PIECES
    moves = [(dw_in.at[pl.ds(n * rows, rows)], dw_buf.at[pl.ds(n * rows, rows)], dw_out.at[pl.ds(n * rows, rows)]) for n in range(PIECES)]
    moves.append((dh_in, dh_buf, dh_out))
    loads = [pltpu.make_async_copy(a, b, load.at[n]) for n, (a, b, _) in enumerate(moves)]
    stores = [pltpu.make_async_copy(b, c, store.at[n]) for n, (_, b, c) in enumerate(moves)]
    for copy in loads:
        copy.start()
    for one, other in zip(loads, stores):
        one.wait()
        other.start()
    for copy in stores:
        copy.wait()


def deliver(grad_hid, grad_w):
    any_spec, dma = pl.BlockSpec(memory_space=pl.ANY), pltpu.SemaphoreType.DMA
    return pl.pallas_call(
        deliver_kernel,
        out_shape=tuple(jax.ShapeDtypeStruct(x.shape, F32) for x in (grad_hid, grad_w)),
        in_specs=[any_spec] * 2,
        out_specs=(any_spec,) * 2,
        scratch_shapes=[pltpu.VMEM((64, DIM), F32), pltpu.VMEM((VOCAB, DIM), F32), dma((PIECES + 1,)), dma((PIECES + 1,))],
        compiler_params=pltpu.CompilerParams(vmem_limit_bytes=67043328),
    )(grad_hid, grad_w)


def prepare(hidden, targets):
    h = hidden.reshape(128, UNITS, ROWS, DIM)
    t = targets.reshape(128, UNITS, ROWS).transpose(1, 0, 2).reshape(UNITS, 8, 128)
    return h, t


def solution(mesh):
    def local_step(hidden, targets, w_blk):
        h, t = prepare(hidden, targets)
        loss, grad_hid, grad_w = fused(h, t, w_blk)
        return loss.reshape(1), *deliver(grad_hid, grad_w)

    return jax.shard_map(
        local_step,
        mesh=mesh,
        in_specs=(P("data", None), P("data"), P("fsdp", None)),
        out_specs=(P("data"), P(("data", "fsdp"), None), P(("data", "fsdp"), None)),
        check_vma=False,
    )
```
